256 devices in a mesh: gx: 16 (over z, core), gy: 16 (over y, x).
Axes of the slice: x: 4, y: 4, z: 8, core: 2. Of those that a mesh axis runs over, the one named last changes fastest.
Arguments:
- velocity: float32 [2, 2048, 2048], P(None, 'gy', 'gx'), may hold values from -6 to 6
- wind_stress: float32 [2, 2048, 2048], P(None, 'gy', 'gx'), may hold values from -6 to 6
- thickness: float32 [2048, 2048], P('gy', 'gx'), may hold values from 0.3 to 3
- ice_mask: int32 [2048, 2048], P('gy', 'gx'), may hold values from 0 to 1
- land_mask: int32 [2048, 2048], P('gy', 'gx'), may hold values from 0 to 1
Outputs:
- velocity_out: float32 [2, 2048, 2048], P(None, 'gy', 'gx')
The draws below stay inside these ranges and needn't reach their ends.
All inputs are finite; a program needn't handle non-finite values.
Results may differ from the reference program's by a relative error of at most 0.0012.
Values sent between devices are 32-bit elements; how exact they have to be, the bound alone decides.
No kernel may reach another device: no remote copies, remote signals or barrier semaphores. Data moves between devices by JAX's collectives and lax.ppermute only.
A program may use at most 64 MiB of HBM per device.

```python
import math
import jax
import jax.numpy as jnp
from jax import lax

CX = 128
CY = 128
PASSES = 2
NX = 2048
NY = 2048


def rectangles(key, count):
    row_ids = lax.broadcasted_iota(jnp.int32, (NY, NX), 0)
    col_ids = lax.broadcasted_iota(jnp.int32, (NY, NX), 1)
    row_least = max(NY // 32, 1)
    row_most = max(NY // 8, row_least + 1)
    col_least = max(NX // 32, 1)
    col_most = max(NX // 8, col_least + 1)
    covered = jnp.zeros((NY, NX), jnp.int32)
    for rect_index in range(count):
        subkeys = jax.random.split(jax.random.fold_in(key, rect_index), 4)
        first_row = jax.random.randint(subkeys[0], (), 0, NY)
        row_span = jax.random.randint(subkeys[1], (), row_least, row_most)
        first_col = jax.random.randint(subkeys[2], (), 0, NX)
        col_span = jax.random.randint(subkeys[3], (), col_least, col_most)
        inside = (row_ids >= first_row) & (row_ids < first_row + row_span) & (col_ids >= first_col) & (col_ids < first_col + col_span)
        covered = jnp.maximum(covered, inside.astype(jnp.int32))
    return covered


def draw_ice_mask(key, part):
    holes = rectangles(jax.random.fold_in(key, 11), 8)
    return (1 - holes).astype(jnp.int32)


def draw_land_mask(key, part):
    return rectangles(jax.random.fold_in(key, 23), 8).astype(jnp.int32)


def draw_wind_stress(key, part):
    base_key = jax.random.fold_in(key, 37)
    return jnp.clip(jax.random.normal(base_key, (2, NY, NX), jnp.float32), -6.0, 6.0)


def levels(key, dims, cuts, smallest, largest):
    gain = 1.0
    for axis_at, parts in cuts:
        draws = jax.random.uniform(jax.random.fold_in(jax.random.fold_in(key, 6), axis_at), (parts,), jnp.float32, smallest / len(cuts), largest / len(cuts))
        gain = gain * jnp.repeat(jnp.exp(draws), dims[axis_at] // parts).reshape((-1,) + (1,) * (len(dims) - 1 - axis_at))
    return gain


def scatter_about(key, shape, scale, bound, cuts=(), dtype=jnp.bfloat16):
    result = scale * jax.random.normal(key, shape, jnp.float32)
    if cuts:
        result = result * levels(key, shape, cuts, -0.22, 0.18)
    return jnp.clip(result, -bound, bound).astype(dtype)


def setup_inputs(seed: int = 0) -> dict:
    streams_of = jax.random.split(jax.random.key(seed), 6)
    return {
        "velocity": scatter_about(streams_of[0], (2, NY, NX), 1.0, 6.0, ((1, 16), (2, 16)), jnp.float32),
        "wind_stress": draw_wind_stress(jax.random.fold_in(streams_of[5], 71), 0),
        "thickness": jnp.clip(jnp.exp(math.log(3.0) - 2.3025851 * jax.random.uniform(streams_of[2], (NY, NX), jnp.float32) ** levels(streams_of[2], (NY, NX), ((0, 16), (1, 16)), -0.2, 0.2)), 0.3, 3.0),
        "ice_mask": draw_ice_mask(jax.random.fold_in(streams_of[5], 71), 0),
        "land_mask": draw_land_mask(jax.random.fold_in(streams_of[5], 71), 0),
    }


CORIOLIS = 1.0
DELTA_MIN = 0.25
WIND_GAIN = 0.2

def shift_below(array, stride, fill_value):
    filler = jnp.full(array.shape[:-1] + (stride,), fill_value, jnp.float32)
    return jnp.concatenate([filler, array[..., :-stride]], axis=-1)

def shift_above(array, stride, fill_value):
    filler = jnp.full(array.shape[:-1] + (stride,), fill_value, jnp.float32)
    return jnp.concatenate([array[..., stride:], filler], axis=-1)

def reduce_lines(lower_band, middle, upper_band, right_side):
    line_total = right_side.shape[-1]
    stride = 1
    while stride < line_total:
        low_lower = shift_below(lower_band, stride, 0.0)
        low_mid = shift_below(middle, stride, 1.0)
        low_upper = shift_below(upper_band, stride, 0.0)
        low_right = shift_below(right_side, stride, 0.0)
        high_lower = shift_above(lower_band, stride, 0.0)
        high_mid = shift_above(middle, stride, 1.0)
        high_upper = shift_above(upper_band, stride, 0.0)
        high_right = shift_above(right_side, stride, 0.0)
        weight_low = -lower_band / low_mid
        weight_high = -upper_band / high_mid
        lower_band, middle, upper_band, right_side = (weight_low * low_lower, middle + weight_low * low_upper + weight_high * high_lower, weight_high * high_upper, right_side + weight_low * low_right + weight_high * high_right)
        stride *= 2
    return right_side / middle

def viscosity_of(u_rim, v_rim, thickness):
    strain_xx = 0.5 * (u_rim[1:-1, 2:] - u_rim[1:-1, :-2])
    strain_yy = 0.5 * (v_rim[2:, 1:-1] - v_rim[:-2, 1:-1])
    shear = 0.25 * (u_rim[2:, 1:-1] - u_rim[:-2, 1:-1] + (v_rim[1:-1, 2:] - v_rim[1:-1, :-2]))
    delta2 = 1.25 * (strain_xx * strain_xx + strain_yy * strain_yy) + shear * shear + 1.5 * strain_xx * strain_yy
    return thickness / (2.0 * jnp.sqrt(delta2 + DELTA_MIN * DELTA_MIN))

def edge_terms(visc_rim):
    centre = visc_rim[1:-1, 1:-1]
    east_edge = jnp.sqrt(centre * visc_rim[1:-1, 2:])
    west_edge = jnp.sqrt(centre * visc_rim[1:-1, :-2])
    north_edge = jnp.sqrt(centre * visc_rim[2:, 1:-1])
    south_edge = jnp.sqrt(centre * visc_rim[:-2, 1:-1])
    return (east_edge, west_edge, north_edge, south_edge)

def u_system(edges, live, ice_mass, weak, press, u_rim, v_speed, wind_x, p_rim):
    east_edge, west_edge, north_edge, south_edge = edges
    centre = ice_mass + east_edge + west_edge + weak * (north_edge + south_edge)
    right_side = ice_mass * u_rim[1:-1, 1:-1] + wind_x + CORIOLIS * ice_mass * v_speed + weak * (north_edge * u_rim[2:, 1:-1] + south_edge * u_rim[:-2, 1:-1]) - 0.5 * press * (p_rim[1:-1, 2:] - p_rim[1:-1, :-2])
    return (jnp.where(live, -west_edge, 0.0), jnp.where(live, centre, 1.0), jnp.where(live, -east_edge, 0.0), jnp.where(live, right_side, 0.0))

def v_system(edges, live, ice_mass, weak, press, v_rim, u_speed, wind_y, p_rim):
    east_edge, west_edge, north_edge, south_edge = edges
    centre = ice_mass + north_edge + south_edge + weak * (east_edge + west_edge)
    right_side = ice_mass * v_rim[1:-1, 1:-1] + wind_y - CORIOLIS * ice_mass * u_speed + weak * (east_edge * v_rim[1:-1, 2:] + west_edge * v_rim[1:-1, :-2]) - 0.5 * press * (p_rim[2:, 1:-1] - p_rim[:-2, 1:-1])
    return (jnp.where(live, -south_edge, 0.0), jnp.where(live, centre, 1.0), jnp.where(live, -north_edge, 0.0), jnp.where(live, right_side, 0.0))

def reference(velocity, wind_stress, thickness, ice_mask, land_mask):
    active = (ice_mask * (1 - land_mask)).astype(jnp.float32)
    live = active > 0.5
    cell_count = float(CX * CY)
    weak = 1.0 / (16.0 * cell_count)
    press = cell_count ** (-0.25)
    drive = WIND_GAIN * cell_count ** (-0.75)
    ice_mass = weak * thickness
    wind_x = drive * wind_stress[0]
    wind_y = drive * wind_stress[1]
    u_speed = velocity[0]
    v_speed = velocity[1]
    p_rim = jnp.pad(thickness, 1)
    for sweep in range(PASSES):
        u_rim = jnp.pad(u_speed, 1)
        v_rim = jnp.pad(v_speed, 1)
        viscosity = viscosity_of(u_rim, v_rim, thickness)
        edges = edge_terms(jnp.pad(viscosity, 1))
        system = u_system(edges, live, ice_mass, weak, press, u_rim, v_speed, wind_x, p_rim)
        u_speed = reduce_lines(*system)
        system = v_system(edges, live, ice_mass, weak, press, v_rim, u_speed, wind_y, p_rim)
        turned = [part.T for part in system]
        v_speed = reduce_lines(*turned).T
    return jnp.stack([u_speed, v_speed])
```

```python
import jax
import jax.numpy as jnp
from jax import lax
from jax.experimental import pallas as pl
from jax.experimental.pallas import tpu as pltpu
from jax.sharding import PartitionSpec as P

CORIOLIS = 1.0
DELTA_MIN = 0.25
WIND_GAIN = 0.2

N = 128
K = 16
TOP = 16
ROWS = N + 2 * TOP
CELLS = float(N * N)
WEAK = 1.0 / (16.0 * CELLS)
PRESS = CELLS ** (-0.25)
DRIVE = WIND_GAIN * CELLS ** (-0.75)
F32 = jnp.float32


def lanes(rows):
    return lax.broadcasted_iota(jnp.int32, (rows, N), 1)


def sublanes(rows):
    return lax.broadcasted_iota(jnp.int32, (rows, N), 0)


def east(own, side):
    a, b = pltpu.roll(own, N - 1, 1), pltpu.roll(side, N - 1, 1)
    last = lanes(own.shape[0]) == N - 1
    return jnp.where(last, b, a), jnp.where(last, a, b)


def west(own, side):
    a, b = pltpu.roll(own, 1, 1), pltpu.roll(side, 1, 1)
    first = lanes(own.shape[0]) == 0
    return jnp.where(first, b, a), jnp.where(first, a, b)


def pick(flag, rows, a, b):
    return jnp.where(jnp.broadcast_to(flag, (rows, N)), a, b)


def pack_columns(vel, wind, thick, ice, land, send_a, send_b, turn):
    live = (ice[...] * (1 - land[...])).astype(F32)
    lane = lanes(N)
    mixed = jnp.where(lane < 36, pltpu.roll(live, 32, 1), vel[0])
    mixed = jnp.where(lane < 28, pltpu.roll(wind[1], 24, 1), mixed)
    mixed = jnp.where(lane < 20, pltpu.roll(thick[...], 16, 1), mixed)
    mixed = jnp.where(lane < 12, pltpu.roll(vel[1], 8, 1), mixed)
    mixed = jnp.where(lane < 4, vel[0], mixed)
    turn[...] = mixed.T
    left = [turn[0:4], turn[8:12], turn[16:20], turn[24:26], turn[32:34]]
    right = [turn[124:128], turn[4:8], turn[12:16], turn[22:24], turn[30:32]]
    even = lax.rem(lax.axis_index("gx"), 2) == 0
    at = 0
    for a, b in zip(left, right):
        n = a.shape[0]
        send_a[at : at + n] = pick(even, n, b, a)
        send_b[at : at + n] = pick(even, n, a, b)
        at += n


def side_columns(got_a, got_b, turn):
    even = lax.rem(lax.axis_index("gx"), 2) == 0
    turn[...] = jnp.zeros((N, N), F32)
    places = ((0, 4, 0, 124), (4, 4, 8, 4), (8, 4, 16, 12), (12, 2, 24, 22), (14, 2, 32, 30))
    for at, n, low, high in places:
        a, b = got_a[at : at + n], got_b[at : at + n]
        turn[low : low + n] = pick(even, n, a, b)
        turn[high : high + n] = pick(even, n, b, a)
    return turn[...].T


def side_field(mixed, slot):
    lane = lanes(N)
    moved = mixed if slot == 0 else pltpu.roll(mixed, N - 8 * slot, 1)
    return jnp.where((lane < 4) | (lane >= 124), moved, 0.0)


def pack_rows(vel, thick, got_a, got_b, send_a, send_b, turn, work):
    mixed = side_columns(got_a, got_b, turn)
    even = lax.rem(lax.axis_index("gy"), 2) == 0
    for k in range(3):
        turn[...] = side_field(mixed, k)
        own = vel.at[k] if k < 2 else thick
        for tile, source in ((0, own), (1, turn)):
            low, high = source[0:2], source[126:128]
            at = 8 * tile + 2 * k
            send_a[at : at + 2] = pick(even, 2, high, low)
            send_b[at : at + 2] = pick(even, 2, low, high)
    for tile in (0, 1):
        send_a[8 * tile + 6 : 8 * tile + 8] = jnp.zeros((2, N), F32)
        send_b[8 * tile + 6 : 8 * tile + 8] = jnp.zeros((2, N), F32)


def root_viscosity(su, sv, st, sh):
    for at in range(TOP - 8, TOP + N + 8, 8):
        here = slice(at, at + 8)
        up, down = slice(at + 1, at + 9), slice(at - 1, at + 7)
        ue, uw = east(su[0, here], su[1, here]), west(su[0, here], su[1, here])
        ve, vw = east(sv[0, here], sv[1, here]), west(sv[0, here], sv[1, here])
        for t in (0, 1):
            strain_xx = 0.5 * (ue[t] - uw[t])
            strain_yy = 0.5 * (sv[t, up] - sv[t, down])
            shear = 0.25 * (su[t, up] - su[t, down] + (ve[t] - vw[t]))
            delta2 = (
                1.25 * (strain_xx * strain_xx + strain_yy * strain_yy)
                + shear * shear
                + 1.5 * strain_xx * strain_yy
            )
            sh[t, here] = jnp.sqrt(st[t, here] / (2.0 * jnp.sqrt(delta2 + DELTA_MIN * DELTA_MIN)))


def systems(su, sv, st, sh, wx, wy, live, tiles, put_u, put_v):
    for at in range(TOP, TOP + N, 8):
        here = slice(at, at + 8)
        up, down = slice(at + 1, at + 9), slice(at - 1, at + 7)
        cell = slice(at - TOP, at - TOP + 8)
        he, hw = east(sh[0, here], sh[1, here]), west(sh[0, here], sh[1, here])
        ve, vw = east(sv[0, here], sv[1, here]), west(sv[0, here], sv[1, here])
        te, tw = east(st[0, here], st[1, here]), west(st[0, here], st[1, here])
        for t in tiles:
            h, thick = sh[t, here], st[t, here]
            e_edge, w_edge = h * he[t], h * hw[t]
            n_edge, s_edge = h * sh[t, up], h * sh[t, down]
            mass = WEAK * thick
            alive = live(t, cell) > 0.5
            if t == 0:
                extra = mass + WEAK * (n_edge + s_edge)
                right = (
                    mass * su[0, here]
                    + DRIVE * wx(cell)
                    + CORIOLIS * mass * sv[0, here]
                    + WEAK * (n_edge * su[0, up] + s_edge * su[0, down])
                    - 0.5 * PRESS * (te[0] - tw[0])
                )
                scale = 1.0 / (extra + e_edge + w_edge)
                put_u(
                    cell,
                    jnp.where(alive, w_edge * scale, 0.0),
                    jnp.where(alive, e_edge * scale, 0.0),
                    jnp.where(alive, extra * scale, 1.0),
                    jnp.where(alive, right * scale, 0.0),
                )
            extra = mass + WEAK * (e_edge + w_edge)
            right = (
                mass * sv[t, here]
                + DRIVE * wy(t, cell)
                + WEAK * (e_edge * ve[t] + w_edge * vw[t])
                - 0.5 * PRESS * (st[t, up] - st[t, down])
            )
            scale = 1.0 / jnp.where(alive, extra + n_edge + s_edge, 1.0)
            put_v(
                t,
                cell,
                jnp.where(alive, s_edge * scale, 0.0),
                jnp.where(alive, n_edge * scale, 0.0),
                jnp.where(alive, extra * scale, 1.0),
                jnp.where(alive, right * scale, 0.0),
                jnp.where(alive, CORIOLIS * mass * scale, 0.0),
            )


def set_rims(bands):
    one, zero = jnp.ones((8, N), F32), jnp.zeros((8, N), F32)
    for half in (0, 1):
        for k in range(4):
            bands[half, k, 0:8] = one if k == 0 else zero
            bands[half, k, 8 + N : 16 + N] = one if k == 1 else zero


def set_band(bands, k, at, value):
    if at + value.shape[0] == N:
        own = sublanes(value.shape[0]) == value.shape[0] - 1
        value = jnp.where(own, 1.0 if k == 1 else 0.0, value)
    bands[0, k, 8 + at : 8 + at + value.shape[0]] = value


def reduce_piece(bands, last, out):
    half, s = 0, 1
    while s < N:
        final = 2 * s >= N
        for at in range(0, N, 8):
            here = slice(8 + at, 16 + at)
            l, u, e, r = (bands[half, k, here] for k in range(4))
            ll, uu, ee, rr = l, u, e, r
            if s < 8 or at >= s:
                low = slice(8 + at - s, 16 + at - s)
                ll = l * bands[half, 0, low]
                ee = ee + l * bands[half, 2, low]
                rr = rr + l * bands[half, 3, low]
            if s < 8 or at + s < N:
                high = slice(8 + at + s, 16 + at + s)
                uu = u * bands[half, 1, high]
                ee = ee + u * bands[half, 2, high]
                rr = rr + u * bands[half, 3, high]
            q = 1.0 / (ll + uu + ee)
            for k, x in enumerate((ll, uu, ee, rr)):
                if final:
                    out(k, at, x * q)
                if not final or at in (0, N - 8):
                    bands[1 - half, k, here] = x * q
        half, s = 1 - half, 2 * s
    row = lambda k, i: bands[half, k, 8 + i : 9 + i]
    lo, uo, eo, ro = last
    lq, uq, eq, rq = (row(k, N - 2) for k in range(4))
    q = 1.0 / (uo + eo + lo * (lq + eq))
    coupling = [row(k, 0) for k in range(4)]
    coupling += [lo * lq * q, uo * q, (eo + lo * eq) * q, (ro + lo * rq) * q]
    second = [row(k, 1) for k in (0, 1, 3)]
    return coupling, second, [lq, uq, rq]


def solve_pieces(got, width, base, me, rowed, halo=None):
    take = lambda k: got[pl.ds(base + k, K, width), :]
    fl, fu, fe, fr, zl, zu, ze, zr = (take(k) for k in range(8))
    nxt = lambda a: pltpu.roll(a, K - 1, 0)
    fe = nxt(fe)
    uu, ee, rr = zu * nxt(fu), ze + zu * fe, zr + zu * nxt(fr)
    q = 1.0 / (zl + ee + uu)
    l, u, e, r = zl * q, uu * q, ee * q, rr * q
    s = 1
    while s < K:
        low = lambda a: pltpu.roll(a, s, 0)
        high = lambda a: pltpu.roll(a, K - s, 0)
        ee = e + l * low(e) + u * high(e)
        rr = r + l * low(r) + u * high(r)
        ll, uu = l * low(l), u * high(u)
        q = 1.0 / (ll + uu + ee)
        l, u, e, r = ll * q, uu * q, ee * q, rr * q
        s *= 2
    rowed[0:K] = jnp.zeros((K, N), F32)
    rowed[K : 2 * K] = r
    rowed[2 * K : 3 * K] = jnp.zeros((K, N), F32)
    before, own = rowed[pl.ds(K - 1 + me, 1), :], rowed[pl.ds(K + me, 1), :]
    if halo is None:
        return before, own
    before2, after = rowed[pl.ds(K - 2 + me, 1), :], rowed[pl.ds(K + 1 + me, 1), :]
    up = jnp.minimum(me + 1, K - 1) * width
    down = jnp.maximum(me - 1, 0) * width
    has_up = jnp.broadcast_to(me < K - 1, (1, N))
    has_down = jnp.broadcast_to(me > 0, (1, N))
    row = lambda at, k: got[pl.ds(at + k, 1), :]
    first = row(up, base + 3) + row(up, base) * own + row(up, base + 1) * after
    first = jnp.where(has_up, first, 0.0)
    second = row(up, halo + 2) + row(up, halo) * own + row(up, halo + 1) * after
    second = jnp.where(has_up, second, 0.0)
    ahead = row(down, halo + 2) + row(down, halo) * before2 + row(down, halo + 1) * before
    ahead = jnp.where(has_down, ahead, 0.0)
    return before, own, ahead, first, second


def spread(dest, me, common, forward, backward, width):
    for d in range(K):
        at = d * width
        dest[at : at + 8 * len(common)] = jnp.concatenate(common, 0) if len(common) > 1 else common[0]
        if forward is not None:
            dest[at + width - 8 : at + width] = pick(me < d, 8, forward, backward)


def tile_of(rows, pad):
    for k, row in enumerate(rows):
        pad[k : k + 1] = row
    return pad[...]


def first_u(vel, wind, thick, ice, land, ca, cb, ra, rb, send, pl_, pu_, pr_, vsys, sth, su, sv, st, sh, turn, tall, bands, pad):
    mixed = side_columns(ca, cb, turn)
    even = lax.rem(lax.axis_index("gy"), 2) == 0
    zero = jnp.zeros((TOP, N), F32)
    for k, s in enumerate((su, sv, st)):
        own = vel.at[k] if k < 2 else thick
        for t in (0, 1):
            s[t, 0:TOP] = zero
            s[t, TOP + N :] = zero
            s[t, TOP : TOP + N] = own[...] if t == 0 else side_field(mixed, k)
            at = 8 * t + 2 * k
            a, b = ra[at : at + 2], rb[at : at + 2]
            s[t, TOP + N : TOP + N + 2] = pick(even, 2, a, b)
            s[t, TOP - 2 : TOP] = pick(even, 2, b, a)
    tall[0] = side_field(mixed, 3)
    tall[1] = side_field(mixed, 4)
    root_viscosity(su, sv, st, sh)

    def live(t, cell):
        if t == 0:
            return (ice[cell] * (1 - land[cell])).astype(F32)
        return tall[1, cell]

    def wy(t, cell):
        return wind[1, cell] if t == 0 else tall[0, cell]

    def put_u(cell, *values):
        for k, x in enumerate(values):
            tall[2 + k, cell] = x

    def put_v(t, cell, *values):
        for k, x in enumerate(values):
            vsys[k, t, cell] = x

    systems(su, sv, st, sh, lambda cell: wind[0, cell], wy, live, (0, 1), put_u, put_v)
    for t in (0, 1):
        sth[t] = st[t]
    last = []
    for k in range(4):
        turned = tall[2 + k].T
        set_band(bands, k, 0, turned)
        last.append(turned[N - 1 :])
    set_rims(bands)
    outs = {0: pl_, 1: pu_, 3: pr_}

    def out(k, at, x):
        if k != 2:
            outs[k][at : at + 8] = x

    main, second, ahead = reduce_piece(bands, last, out)
    me = lax.axis_index("gx")
    common = tile_of(main, pad)
    pad[...] = jnp.zeros((8, N), F32)
    forward = tile_of(ahead, pad)
    backward = tile_of(second, pad)
    spread(send, me, [common], forward, backward, 16)


def load_v(bands, vsys, t, speed):
    last = []
    for k in range(4):
        x = vsys[k, t]
        if k == 3:
            x = x - vsys[4, t] * speed
        set_band(bands, k, 0, x)
        last.append(x[N - 1 :])
    set_rims(bands)
    return last


def first_v(got, pl_, pu_, pr_, vsys, send, u_new, vp, turn, bands, pad, rowed):
    me = lax.axis_index("gx")
    before, own, ahead, first, second = solve_pieces(got, 16, 0, me, rowed, 8)
    turn[...] = pr_[...] + pl_[...] * before + pu_[...] * own
    u_new[0] = turn[...].T
    turn[...] = jnp.zeros((N, N), F32)
    turn[0:1] = first
    turn[1:2] = second
    turn[N - 2 : N - 1] = ahead
    turn[N - 1 : N] = before
    u_new[1] = turn[...].T
    mains = []
    for t in (0, 1):
        last = load_v(bands, vsys, t, u_new[t])

        def out(k, at, x):
            if k != 2:
                vp[min(k, 2), t, at : at + 8] = x

        main, second, ahead = reduce_piece(bands, last, out)
        mains.append(tile_of(main, pad))
        if t == 0:
            extras = (ahead, second)
    pad[...] = jnp.zeros((8, N), F32)
    last_rows = [u_new[0, N - 2 : N - 1], u_new[0, N - 1 : N], u_new[1, N - 1 : N]]
    first_rows = [u_new[0, 1:2], u_new[0, 0:1], u_new[1, 0:1]]
    forward = tile_of(extras[0] + last_rows, pad)
    backward = tile_of(extras[1] + first_rows, pad)
    spread(send, lax.axis_index("gy"), mains, forward, backward, 24)


def second_u(got, vp, u_new, sth, wind, ice, land, send, pl_, pu_, pr_, vsys, su, sv, sh, tall, bands, pad, rowed):
    me = lax.axis_index("gy")
    up = jnp.minimum(me + 1, K - 1) * 24
    down = jnp.maximum(me - 1, 0) * 24
    has_up = jnp.broadcast_to(me < K - 1, (1, N))
    has_down = jnp.broadcast_to(me > 0, (1, N))
    zero = jnp.zeros((TOP, N), F32)
    for t in (0, 1):
        before, own, ahead, first, second = solve_pieces(got, 24, 8 * t, me, rowed, 16)
        for s in (su, sv):
            s[t, 0:TOP] = zero
            s[t, TOP + N :] = zero
        sv[t, TOP : TOP + N] = vp[2, t] + vp[0, t] * before + vp[1, t] * own
        sv[t, TOP - 1 : TOP] = before
        sv[t, TOP + N : TOP + N + 1] = first
        su[t, TOP : TOP + N] = u_new[t]
        near = 20 if t == 0 else 21
        row = lambda at, k: got[pl.ds(at + k, 1), :]
        su[t, TOP - 1 : TOP] = jnp.where(has_down, row(down, near), 0.0)
        su[t, TOP + N : TOP + N + 1] = jnp.where(has_up, row(up, near), 0.0)
        if t == 0:
            sv[0, TOP - 2 : TOP - 1] = ahead
            sv[0, TOP + N + 1 : TOP + N + 2] = second
            su[0, TOP - 2 : TOP - 1] = jnp.where(has_down, row(down, 19), 0.0)
            su[0, TOP + N + 1 : TOP + N + 2] = jnp.where(has_up, row(up, 19), 0.0)
    root_viscosity(su, sv, sth, sh)

    def live(t, cell):
        return (ice[cell] * (1 - land[cell])).astype(F32)

    def put_u(cell, *values):
        for k, x in enumerate(values):
            tall[k, cell] = x

    def put_v(t, cell, *values):
        for k, x in enumerate(values):
            vsys[k, t, cell] = x

    systems(su, sv, sth, sh, lambda cell: wind[0, cell], lambda t, cell: wind[1, cell], live, (0,), put_u, put_v)
    last = []
    for k in range(4):
        turned = tall[k].T
        set_band(bands, k, 0, turned)
        last.append(turned[N - 1 :])
    set_rims(bands)
    outs = {0: pl_, 1: pu_, 3: pr_}

    def out(k, at, x):
        if k != 2:
            outs[k][at : at + 8] = x

    main, _, _ = reduce_piece(bands, last, out)
    spread(send, lax.axis_index("gx"), [tile_of(main, pad)], None, None, 8)


def second_v(got, pl_, pu_, pr_, vsys, send, u_new, vp, turn, bands, pad, rowed):
    before, own = solve_pieces(got, 8, 0, lax.axis_index("gx"), rowed)
    turn[...] = pr_[...] + pl_[...] * before + pu_[...] * own
    u_new[...] = turn[...].T
    last = load_v(bands, vsys, 0, u_new[...])

    def out(k, at, x):
        if k != 2:
            vp[min(k, 2), at : at + 8] = x

    main, _, _ = reduce_piece(bands, last, out)
    spread(send, lax.axis_index("gy"), [tile_of(main, pad)], None, None, 8)


def finish(got, vp, u_new, out, rowed):
    before, own = solve_pieces(got, 8, 0, lax.axis_index("gy"), rowed)
    out[0] = u_new[...]
    out[1] = vp[2] + vp[0] * before + vp[1] * own


def call(kernel, outs, scratch, *args):
    vmem = pl.BlockSpec(memory_space=pltpu.VMEM)
    shapes = [jax.ShapeDtypeStruct(s, F32) for s in outs]
    return pl.pallas_call(
        kernel,
        out_shape=shapes,
        in_specs=[vmem] * len(args),
        out_specs=[vmem] * len(outs),
        scratch_shapes=[pltpu.VMEM(s, F32) for s in scratch],
    )(*args)


def neighbours(a, b, axis):
    inner = [(i, i ^ 1) for i in range(K)]
    outer = [p for i in range(1, K - 1, 2) for p in ((i, i + 1), (i + 1, i))]
    return lax.ppermute(a, axis, inner), lax.ppermute(b, axis, outer)


def share(rows, axis):
    width = rows.shape[0] // K
    moved = lax.all_to_all(rows.reshape(K, width, N), axis, 0, 0, tiled=True)
    return moved.reshape(K * width, N)


def on_device(velocity, wind, thick, ice, land):
    square, halves, rim = (N, N), (2, N, N), (2, ROWS, N)
    bands, pad, rowed = (2, 4, N + 16, N), (8, N), (3 * K, N)
    a, b = call(pack_columns, [(16, N)] * 2, [square], velocity, wind, thick, ice, land)
    ca, cb = neighbours(a, b, "gx")
    a, b = call(pack_rows, [(16, N)] * 2, [square, pad], velocity, thick, ca, cb)
    ra, rb = neighbours(a, b, "gy")
    send, l, u, r, vsys, sth = call(
        first_u,
        [(K * 16, N), square, square, square, (5,) + halves, rim],
        [rim] * 4 + [square, (6, N, N), bands, pad],
        velocity, wind, thick, ice, land, ca, cb, ra, rb,
    )
    got = share(send, "gx")
    send, u_new, vp = call(
        first_v,
        [(K * 24, N), halves, (3,) + halves],
        [square, bands, pad, rowed],
        got, l, u, r, vsys,
    )
    got = share(send, "gy")
    send, l, u, r, vsys = call(
        second_u,
        [(K * 8, N), square, square, square, (5, 1, N, N)],
        [rim] * 3 + [(4, N, N), bands, pad, rowed],
        got, vp, u_new, sth, wind, ice, land,
    )
    got = share(send, "gx")
    send, u_new, vp = call(
        second_v,
        [(K * 8, N), square, (3, N, N)],
        [square, bands, pad, rowed],
        got, l, u, r, vsys,
    )
    got = share(send, "gy")
    (out,) = call(finish, [halves], [rowed], got, vp, u_new)
    return out


def solution(mesh):
    field = P(None, "gy", "gx")
    flat = P("gy", "gx")
    return jax.shard_map(
        on_device,
        mesh=mesh,
        in_specs=(field, field, flat, flat, flat),
        out_specs=field,
        check_vma=False,
    )
```

```python
import jax
import jax.numpy as jnp
from jax import lax
from jax.experimental import pallas as pl
from jax.experimental.pallas import tpu as pltpu
from jax.sharding import PartitionSpec as P

CORIOLIS = 1.0
DELTA_MIN = 0.25
WIND_GAIN = 0.2

N = 128
K = 16
TOP = 16
ROWS = N + 2 * TOP
CELLS = float(N * N)
WEAK = 1.0 / (16.0 * CELLS)
PRESS = CELLS ** (-0.25)
DRIVE = WIND_GAIN * CELLS ** (-0.75)
F32 = jnp.float32


def lanes(rows):
    return lax.broadcasted_iota(jnp.int32, (rows, N), 1)


def sublanes(rows):
    return lax.broadcasted_iota(jnp.int32, (rows, N), 0)


def east(own, side):
    a, b = pltpu.roll(own, N - 1, 1), pltpu.roll(side, N - 1, 1)
    last = lanes(own.shape[0]) == N - 1
    return jnp.where(last, b, a), jnp.where(last, a, b)


def west(own, side):
    a, b = pltpu.roll(own, 1, 1), pltpu.roll(side, 1, 1)
    first = lanes(own.shape[0]) == 0
    return jnp.where(first, b, a), jnp.where(first, a, b)


def pick(flag, rows, a, b):
    return jnp.where(jnp.broadcast_to(flag, (rows, N)), a, b)


def pack_columns(vel, wind, thick, ice, land, send_a, send_b, turn):
    live = (ice[...] * (1 - land[...])).astype(F32)
    lane = lanes(N)
    mixed = jnp.where(lane < 36, pltpu.roll(live, 32, 1), vel[0])
    mixed = jnp.where(lane < 28, pltpu.roll(wind[1], 24, 1), mixed)
    mixed = jnp.where(lane < 20, pltpu.roll(thick[...], 16, 1), mixed)
    mixed = jnp.where(lane < 12, pltpu.roll(vel[1], 8, 1), mixed)
    mixed = jnp.where(lane < 4, vel[0], mixed)
    turn[...] = mixed.T
    left = [turn[0:4], turn[8:12], turn[16:20], turn[24:26], turn[32:34]]
    right = [turn[124:128], turn[4:8], turn[12:16], turn[22:24], turn[30:32]]
    even = lax.rem(lax.axis_index("gx"), 2) == 0
    at = 0
    for a, b in zip(left, right):
        n = a.shape[0]
        send_a[at : at + n] = pick(even, n, b, a)
        send_b[at : at + n] = pick(even, n, a, b)
        at += n


def side_columns(got_a, got_b, turn):
    even = lax.rem(lax.axis_index("gx"), 2) == 0
    turn[...] = jnp.zeros((N, N), F32)
    places = ((0, 4, 0, 124), (4, 4, 8, 4), (8, 4, 16, 12), (12, 2, 24, 22), (14, 2, 32, 30))
    for at, n, low, high in places:
        a, b = got_a[at : at + n], got_b[at : at + n]
        turn[low : low + n] = pick(even, n, a, b)
        turn[high : high + n] = pick(even, n, b, a)
    return turn[...].T


def side_field(mixed, slot):
    lane = lanes(N)
    moved = mixed if slot == 0 else pltpu.roll(mixed, N - 8 * slot, 1)
    return jnp.where((lane < 4) | (lane >= 124), moved, 0.0)


def pack_rows(vel, thick, got_a, got_b, send_a, send_b, turn, work):
    mixed = side_columns(got_a, got_b, turn)
    even = lax.rem(lax.axis_index("gy"), 2) == 0
    for k in range(3):
        turn[...] = side_field(mixed, k)
        own = vel.at[k] if k < 2 else thick
        for tile, source in ((0, own), (1, turn)):
            low, high = source[0:2], source[126:128]
            at = 8 * tile + 2 * k
            send_a[at : at + 2] = pick(even, 2, high, low)
            send_b[at : at + 2] = pick(even, 2, low, high)
    for tile in (0, 1):
        send_a[8 * tile + 6 : 8 * tile + 8] = jnp.zeros((2, N), F32)
        send_b[8 * tile + 6 : 8 * tile + 8] = jnp.zeros((2, N), F32)


def root_viscosity(su, sv, st, sh):
    for at in range(TOP - 8, TOP + N + 8, 8):
        here = slice(at, at + 8)
        up, down = slice(at + 1, at + 9), slice(at - 1, at + 7)
        ue, uw = east(su[0, here], su[1, here]), west(su[0, here], su[1, here])
        ve, vw = east(sv[0, here], sv[1, here]), west(sv[0, here], sv[1, here])
        for t in (0, 1):
            strain_xx = 0.5 * (ue[t] - uw[t])
            strain_yy = 0.5 * (sv[t, up] - sv[t, down])
            shear = 0.25 * (su[t, up] - su[t, down] + (ve[t] - vw[t]))
            delta2 = (
                1.25 * (strain_xx * strain_xx + strain_yy * strain_yy)
                + shear * shear
                + 1.5 * strain_xx * strain_yy
            )
            sh[t, here] = jnp.sqrt(st[t, here] / (2.0 * jnp.sqrt(delta2 + DELTA_MIN * DELTA_MIN)))


def systems(su, sv, st, sh, wx, wy, live, tiles, put_u, put_v):
    for at in range(TOP, TOP + N, 8):
        here = slice(at, at + 8)
        up, down = slice(at + 1, at + 9), slice(at - 1, at + 7)
        cell = slice(at - TOP, at - TOP + 8)
        he, hw = east(sh[0, here], sh[1, here]), west(sh[0, here], sh[1, here])
        ve, vw = east(sv[0, here], sv[1, here]), west(sv[0, here], sv[1, here])
        te, tw = east(st[0, here], st[1, here]), west(st[0, here], st[1, here])
        for t in tiles:
            h, thick = sh[t, here], st[t, here]
            e_edge, w_edge = h * he[t], h * hw[t]
            n_edge, s_edge = h * sh[t, up], h * sh[t, down]
            mass = WEAK * thick
            alive = live(t, cell) > 0.5
            if t == 0:
                extra = mass + WEAK * (n_edge + s_edge)
                right = (
                    mass * su[0, here]
                    + DRIVE * wx(cell)
                    + CORIOLIS * mass * sv[0, here]
                    + WEAK * (n_edge * su[0, up] + s_edge * su[0, down])
                    - 0.5 * PRESS * (te[0] - tw[0])
                )
                scale = 1.0 / (extra + e_edge + w_edge)
                put_u(
                    cell,
                    jnp.where(alive, w_edge * scale, 0.0),
                    jnp.where(alive, e_edge * scale, 0.0),
                    jnp.where(alive, extra * scale, 1.0),
                    jnp.where(alive, right * scale, 0.0),
                )
            extra = mass + WEAK * (e_edge + w_edge)
            right = (
                mass * sv[t, here]
                + DRIVE * wy(t, cell)
                + WEAK * (e_edge * ve[t] + w_edge * vw[t])
                - 0.5 * PRESS * (st[t, up] - st[t, down])
            )
            scale = 1.0 / jnp.where(alive, extra + n_edge + s_edge, 1.0)
            put_v(
                t,
                cell,
                jnp.where(alive, s_edge * scale, 0.0),
                jnp.where(alive, n_edge * scale, 0.0),
                jnp.where(alive, extra * scale, 1.0),
                jnp.where(alive, right * scale, 0.0),
                jnp.where(alive, CORIOLIS * mass * scale, 0.0),
            )


def set_rims(bands):
    one, zero = jnp.ones((8, N), F32), jnp.zeros((8, N), F32)
    for half in (0, 1):
        for k in range(4):
            bands[half, k, 0:8] = one if k == 0 else zero
            bands[half, k, 8 + N : 16 + N] = one if k == 1 else zero


def set_band(bands, k, at, value):
    if at + value.shape[0] == N:
        own = sublanes(value.shape[0]) == value.shape[0] - 1
        value = jnp.where(own, 1.0 if k == 1 else 0.0, value)
    bands[0, k, 8 + at : 8 + at + value.shape[0]] = value


def reduce_piece(bands, last, out):
    half, s = 0, 1
    while s < N:
        final = 2 * s >= N
        for at in range(0, N, 8):
            here = slice(8 + at, 16 + at)
            l, u, e, r = (bands[half, k, here] for k in range(4))
            ll, uu, ee, rr = l, u, e, r
            if s < 8 or at >= s:
                low = slice(8 + at - s, 16 + at - s)
                ll = l * bands[half, 0, low]
                ee = ee + l * bands[half, 2, low]
                rr = rr + l * bands[half, 3, low]
            if s < 8 or at + s < N:
                high = slice(8 + at + s, 16 + at + s)
                uu = u * bands[half, 1, high]
                ee = ee + u * bands[half, 2, high]
                rr = rr + u * bands[half, 3, high]
            q = 1.0 / (ll + uu + ee)
            for k, x in enumerate((ll, uu, ee, rr)):
                if final:
                    out(k, at, x * q)
                if not final or at in (0, N - 8):
                    bands[1 - half, k, here] = x * q
        half, s = 1 - half, 2 * s
    row = lambda k, i: bands[half, k, 8 + i : 9 + i]
    lo, uo, eo, ro = last
    lq, uq, eq, rq = (row(k, N - 2) for k in range(4))
    q = 1.0 / (uo + eo + lo * (lq + eq))
    coupling = [row(k, 0) for k in range(4)]
    coupling += [lo * lq * q, uo * q, (eo + lo * eq) * q, (ro + lo * rq) * q]
    second = [row(k, 1) for k in (0, 1, 3)]
    return coupling, second, [lq, uq, rq]


def solve_pieces(got, width, base, me, rowed, halo=None):
    take = lambda k: got[pl.ds(base + k, K, width), :]
    fl, fu, fe, fr, zl, zu, ze, zr = (take(k) for k in range(8))
    nxt = lambda a: pltpu.roll(a, K - 1, 0)
    fe = nxt(fe)
    uu, ee, rr = zu * nxt(fu), ze + zu * fe, zr + zu * nxt(fr)
    q = 1.0 / (zl + ee + uu)
    l, u, e, r = zl * q, uu * q, ee * q, rr * q
    s = 1
    while s < K:
        low = lambda a: pltpu.roll(a, s, 0)
        high = lambda a: pltpu.roll(a, K - s, 0)
        ee = e + l * low(e) + u * high(e)
        rr = r + l * low(r) + u * high(r)
        ll, uu = l * low(l), u * high(u)
        q = 1.0 / (ll + uu + ee)
        l, u, e, r = ll * q, uu * q, ee * q, rr * q
        s *= 2
    rowed[0:K] = jnp.zeros((K, N), F32)
    rowed[K : 2 * K] = r
    rowed[2 * K : 3 * K] = jnp.zeros((K, N), F32)
    before, own = rowed[pl.ds(K - 1 + me, 1), :], rowed[pl.ds(K + me, 1), :]
    if halo is None:
        return before, own
    before2, after = rowed[pl.ds(K - 2 + me, 1), :], rowed[pl.ds(K + 1 + me, 1), :]
    up = jnp.minimum(me + 1, K - 1) * width
    down = jnp.maximum(me - 1, 0) * width
    has_up = jnp.broadcast_to(me < K - 1, (1, N))
    has_down = jnp.broadcast_to(me > 0, (1, N))
    row = lambda at, k: got[pl.ds(at + k, 1), :]
    first = row(up, base + 3) + row(up, base) * own + row(up, base + 1) * after
    first = jnp.where(has_up, first, 0.0)
    second = row(up, halo + 2) + row(up, halo) * own + row(up, halo + 1) * after
    second = jnp.where(has_up, second, 0.0)
    ahead = row(down, halo + 2) + row(down, halo) * before2 + row(down, halo + 1) * before
    ahead = jnp.where(has_down, ahead, 0.0)
    return before, own, ahead, first, second


def spread(dest, me, common, forward, backward, width):
    for d in range(K):
        at = d * width
        dest[at : at + 8 * len(common)] = jnp.concatenate(common, 0) if len(common) > 1 else common[0]
        if forward is not None:
            dest[at + width - 8 : at + width] = pick(me < d, 8, forward, backward)


def tile_of(rows, pad):
    for k, row in enumerate(rows):
        pad[k : k + 1] = row
    return pad[...]


def first_u(vel, wind, thick, ice, land, ca, cb, ra, rb, send, pl_, pu_, pr_, vsys, sth, su, sv, st, sh, turn, tall, bands, pad):
    mixed = side_columns(ca, cb, turn)
    even = lax.rem(lax.axis_index("gy"), 2) == 0
    zero = jnp.zeros((TOP, N), F32)
    for k, s in enumerate((su, sv, st)):
        own = vel.at[k] if k < 2 else thick
        for t in (0, 1):
            s[t, 0:TOP] = zero
            s[t, TOP + N :] = zero
            s[t, TOP : TOP + N] = own[...] if t == 0 else side_field(mixed, k)
            at = 8 * t + 2 * k
            a, b = ra[at : at + 2], rb[at : at + 2]
            s[t, TOP + N : TOP + N + 2] = pick(even, 2, a, b)
            s[t, TOP - 2 : TOP] = pick(even, 2, b, a)
    tall[0] = side_field(mixed, 3)
    tall[1] = side_field(mixed, 4)
    root_viscosity(su, sv, st, sh)

    def live(t, cell):
        if t == 0:
            return (ice[cell] * (1 - land[cell])).astype(F32)
        return tall[1, cell]

    def wy(t, cell):
        return wind[1, cell] if t == 0 else tall[0, cell]

    def put_u(cell, *values):
        for k, x in enumerate(values):
            tall[2 + k, cell] = x

    def put_v(t, cell, *values):
        for k, x in enumerate(values):
            vsys[k, t, cell] = x

    systems(su, sv, st, sh, lambda cell: wind[0, cell], wy, live, (0, 1), put_u, put_v)
    for t in (0, 1):
        sth[t] = st[t]
    last = []
    for k in range(4):
        turned = tall[2 + k].T
        set_band(bands, k, 0, turned)
        last.append(turned[N - 1 :])
    set_rims(bands)
    outs = {0: pl_, 1: pu_, 3: pr_}

    def out(k, at, x):
        if k != 2:
            outs[k][at : at + 8] = x

    main, second, ahead = reduce_piece(bands, last, out)
    me = lax.axis_index("gx")
    common = tile_of(main, pad)
    pad[...] = jnp.zeros((8, N), F32)
    forward = tile_of(ahead, pad)
    backward = tile_of(second, pad)
    spread(send, me, [common], forward, backward, 16)


def load_v(bands, vsys, t, speed):
    last = []
    for k in range(4):
        x = vsys[k, t]
        if k == 3:
            x = x - vsys[4, t] * speed
        set_band(bands, k, 0, x)
        last.append(x[N - 1 :])
    set_rims(bands)
    return last


def first_v(got, pl_, pu_, pr_, vsys, send, u_new, vp, turn, bands, pad, rowed):
    me = lax.axis_index("gx")
    before, own, ahead, first, second = solve_pieces(got, 16, 0, me, rowed, 8)
    turn[...] = pr_[...] + pl_[...] * before + pu_[...] * own
    u_new[0] = turn[...].T
    turn[...] = jnp.zeros((N, N), F32)
    turn[0:1] = first
    turn[1:2] = second
    turn[N - 2 : N - 1] = ahead
    turn[N - 1 : N] = before
    u_new[1] = turn[...].T
    mains = []
    for t in (0, 1):
        last = load_v(bands, vsys, t, u_new[t])

        def out(k, at, x):
            if k != 2:
                vp[min(k, 2), t, at : at + 8] = x

        main, second, ahead = reduce_piece(bands, last, out)
        mains.append(tile_of(main, pad))
        if t == 0:
            extras = (ahead, second)
    pad[...] = jnp.zeros((8, N), F32)
    last_rows = [u_new[0, N - 2 : N - 1], u_new[0, N - 1 : N], u_new[1, N - 1 : N]]
    first_rows = [u_new[0, 1:2], u_new[0, 0:1], u_new[1, 0:1]]
    forward = tile_of(extras[0] + last_rows, pad)
    backward = tile_of(extras[1] + first_rows, pad)
    spread(send, lax.axis_index("gy"), mains, forward, backward, 24)


def second_u(got, vp, u_new, sth, wind, ice, land, send, pl_, pu_, pr_, vsys, su, sv, sh, tall, bands, pad, rowed):
    me = lax.axis_index("gy")
    up = jnp.minimum(me + 1, K - 1) * 24
    down = jnp.maximum(me - 1, 0) * 24
    has_up = jnp.broadcast_to(me < K - 1, (1, N))
    has_down = jnp.broadcast_to(me > 0, (1, N))
    zero = jnp.zeros((TOP, N), F32)
    for t in (0, 1):
        before, own, ahead, first, second = solve_pieces(got, 24, 8 * t, me, rowed, 16)
        for s in (su, sv):
            s[t, 0:TOP] = zero
            s[t, TOP + N :] = zero
        sv[t, TOP : TOP + N] = vp[2, t] + vp[0, t] * before + vp[1, t] * own
        sv[t, TOP - 1 : TOP] = before
        sv[t, TOP + N : TOP + N + 1] = first
        su[t, TOP : TOP + N] = u_new[t]
        near = 20 if t == 0 else 21
        row = lambda at, k: got[pl.ds(at + k, 1), :]
        su[t, TOP - 1 : TOP] = jnp.where(has_down, row(down, near), 0.0)
        su[t, TOP + N : TOP + N + 1] = jnp.where(has_up, row(up, near), 0.0)
        if t == 0:
            sv[0, TOP - 2 : TOP - 1] = ahead
            sv[0, TOP + N + 1 : TOP + N + 2] = second
            su[0, TOP - 2 : TOP - 1] = jnp.where(has_down, row(down, 19), 0.0)
            su[0, TOP + N + 1 : TOP + N + 2] = jnp.where(has_up, row(up, 19), 0.0)
    root_viscosity(su, sv, sth, sh)

    def live(t, cell):
        return (ice[cell] * (1 - land[cell])).astype(F32)

    def put_u(cell, *values):
        for k, x in enumerate(values):
            tall[k, cell] = x

    def put_v(t, cell, *values):
        for k, x in enumerate(values):
            vsys[k, t, cell] = x

    systems(su, sv, sth, sh, lambda cell: wind[0, cell], lambda t, cell: wind[1, cell], live, (0,), put_u, put_v)
    last = []
    for k in range(4):
        turned = tall[k].T
        set_band(bands, k, 0, turned)
        last.append(turned[N - 1 :])
    set_rims(bands)
    outs = {0: pl_, 1: pu_, 3: pr_}

    def out(k, at, x):
        if k != 2:
            outs[k][at : at + 8] = x

    main, _, _ = reduce_piece(bands, last, out)
    spread(send, lax.axis_index("gx"), [tile_of(main, pad)], None, None, 8)


def second_v(got, pl_, pu_, pr_, vsys, send, u_new, vp, turn, bands, pad, rowed):
    before, own = solve_pieces(got, 8, 0, lax.axis_index("gx"), rowed)
    turn[...] = pr_[...] + pl_[...] * before + pu_[...] * own
    u_new[...] = turn[...].T
    last = load_v(bands, vsys, 0, u_new[...])

    def out(k, at, x):
        if k != 2:
            vp[min(k, 2), at : at + 8] = x

    main, _, _ = reduce_piece(bands, last, out)
    spread(send, lax.axis_index("gy"), [tile_of(main, pad)], None, None, 8)


def finish(got, vp, u_new, out, rowed):
    before, own = solve_pieces(got, 8, 0, lax.axis_index("gy"), rowed)
    out[0] = u_new[...]
    out[1] = vp[2] + vp[0] * before + vp[1] * own


def call(kernel, outs, scratch, *args):
    vmem = pl.BlockSpec(memory_space=pltpu.VMEM)
    shapes = [jax.ShapeDtypeStruct(s, F32) for s in outs]
    return pl.pallas_call(
        kernel,
        out_shape=shapes,
        in_specs=[vmem] * len(args),
        out_specs=[vmem] * len(outs),
        scratch_shapes=[pltpu.VMEM(s, F32) for s in scratch],
        compiler_params=pltpu.CompilerParams(vmem_limit_bytes=8 * 1024 * 1024),
    )(*args)


def neighbours(a, b, axis):
    inner = [(i, i ^ 1) for i in range(K)]
    outer = [p for i in range(1, K - 1, 2) for p in ((i, i + 1), (i + 1, i))]
    return lax.ppermute(a, axis, inner), lax.ppermute(b, axis, outer)


def share(rows, axis):
    width = rows.shape[0] // K
    moved = lax.all_to_all(rows.reshape(K, width, N), axis, 0, 0, tiled=True)
    return moved.reshape(K * width, N)


def on_device(velocity, wind, thick, ice, land):
    square, halves, rim = (N, N), (2, N, N), (2, ROWS, N)
    bands, pad, rowed = (2, 4, N + 16, N), (8, N), (3 * K, N)
    a, b = call(pack_columns, [(16, N)] * 2, [square], velocity, wind, thick, ice, land)
    ca, cb = neighbours(a, b, "gx")
    a, b = call(pack_rows, [(16, N)] * 2, [square, pad], velocity, thick, ca, cb)
    ra, rb = neighbours(a, b, "gy")
    send, l, u, r, vsys, sth = call(
        first_u,
        [(K * 16, N), square, square, square, (5,) + halves, rim],
        [rim] * 4 + [square, (6, N, N), bands, pad],
        velocity, wind, thick, ice, land, ca, cb, ra, rb,
    )
    got = share(send, "gx")
    send, u_new, vp = call(
        first_v,
        [(K * 24, N), halves, (3,) + halves],
        [square, bands, pad, rowed],
        got, l, u, r, vsys,
    )
    got = share(send, "gy")
    send, l, u, r, vsys = call(
        second_u,
        [(K * 8, N), square, square, square, (5, 1, N, N)],
        [rim] * 3 + [(4, N, N), bands, pad, rowed],
        got, vp, u_new, sth, wind, ice, land,
    )
    got = share(send, "gx")
    send, u_new, vp = call(
        second_v,
        [(K * 8, N), square, (3, N, N)],
        [square, bands, pad, rowed],
        got, l, u, r, vsys,
    )
    got = share(send, "gy")
    (out,) = call(finish, [halves], [rowed], got, vp, u_new)
    return out


def solution(mesh):
    field = P(None, "gy", "gx")
    flat = P("gy", "gx")
    return jax.shard_map(
        on_device,
        mesh=mesh,
        in_specs=(field, field, flat, flat, flat),
        out_specs=field,
        check_vma=False,
    )
```

```python
import jax
import jax.numpy as jnp
from jax import lax
from jax.experimental import pallas as pl
from jax.experimental.pallas import tpu as pltpu
from jax.sharding import PartitionSpec as P

CORIOLIS = 1.0
DELTA_MIN = 0.25
WIND_GAIN = 0.2

N = 128
K = 16
TOP = 16
ROWS = N + 2 * TOP
CELLS = float(N * N)
WEAK = 1.0 / (16.0 * CELLS)
PRESS = CELLS ** (-0.25)
DRIVE = WIND_GAIN * CELLS ** (-0.75)
F32 = jnp.float32


def lanes(rows):
    return lax.broadcasted_iota(jnp.int32, (rows, N), 1)


def sublanes(rows):
    return lax.broadcasted_iota(jnp.int32, (rows, N), 0)


def east(own, side):
    a, b = pltpu.roll(own, N - 1, 1), pltpu.roll(side, N - 1, 1)
    last = lanes(own.shape[0]) == N - 1
    return jnp.where(last, b, a), jnp.where(last, a, b)


def west(own, side):
    a, b = pltpu.roll(own, 1, 1), pltpu.roll(side, 1, 1)
    first = lanes(own.shape[0]) == 0
    return jnp.where(first, b, a), jnp.where(first, a, b)


def pick(flag, rows, a, b):
    return jnp.where(jnp.broadcast_to(flag, (rows, N)), a, b)


def edge_rows(vel, thick, send_a, send_b, low, high, sems):
    copies = []
    for k in range(3):
        source = vel.at[k] if k < 2 else thick
        copies.append(pltpu.make_async_copy(source.at[0:8], low.at[k], sems.at[2 * k]))
        copies.append(pltpu.make_async_copy(source.at[N - 8 : N], high.at[k], sems.at[2 * k + 1]))
    for c in copies:
        c.start()
    for c in copies:
        c.wait()
    even = lax.rem(lax.axis_index("gy"), 2) == 0
    for k in range(3):
        first, final = low[k, 0:2], high[k, 6:8]
        send_a[2 * k : 2 * k + 2] = pick(even, 2, final, first)
        send_b[2 * k : 2 * k + 2] = pick(even, 2, first, final)
    send_a[6:8] = jnp.zeros((2, N), F32)
    send_b[6:8] = jnp.zeros((2, N), F32)


def load(vel, wind, thick, ice, land, vel_v, wind_v, thick_v, live_v, edges, ice_v, land_v, turn, sems):
    pairs = ((vel, vel_v), (thick, thick_v), (ice, ice_v), (land, land_v), (wind, wind_v))
    copies = [pltpu.make_async_copy(x, y, sems.at[k]) for k, (x, y) in enumerate(pairs)]
    for c in copies:
        c.start()
    for c in copies:
        c.wait()
    live = (ice_v[...] * (1 - land_v[...])).astype(F32)
    live_v[...] = live
    lane = lanes(N)
    mixed = jnp.where(lane < 36, pltpu.roll(live, 32, 1), vel_v[0])
    mixed = jnp.where(lane < 28, pltpu.roll(wind_v[1], 24, 1), mixed)
    mixed = jnp.where(lane < 20, pltpu.roll(thick_v[...], 16, 1), mixed)
    mixed = jnp.where(lane < 12, pltpu.roll(vel_v[1], 8, 1), mixed)
    mixed = jnp.where(lane < 4, vel_v[0], mixed)
    turn[...] = mixed.T
    left = ((0, 4), (8, 4), (16, 4), (24, 2), (32, 2))
    right = ((124, 4), (4, 4), (12, 4), (22, 2), (30, 2))
    for base, places in ((0, left), (16, right)):
        for at, n in places:
            edges[base : base + n] = turn[at : at + n]
            base += n


def both_ways(a, b, axis):
    even = lax.rem(lax.axis_index(axis), 2) == 0
    n = a.shape[0]
    return pick(even, n, a, b), pick(even, n, b, a)


def pack_columns(edges, ra, rb, send_a, send_b, turn):
    turn[...] = jnp.zeros((N, N), F32)
    for k in range(3):
        above, below = both_ways(ra[2 * k : 2 * k + 2], rb[2 * k : 2 * k + 2], "gy")
        turn[4 * k : 4 * k + 2] = below
        turn[4 * k + 2 : 4 * k + 4] = above
    turn[...] = turn[...].T
    even = lax.rem(lax.axis_index("gx"), 2) == 0
    for at, n, left, right in (
        (0, 16, edges[0:16], edges[16:32]),
        (16, 4, turn[0:4], turn[N - 4 : N]),
        (20, 4, jnp.zeros((4, N), F32), jnp.zeros((4, N), F32)),
    ):
        send_a[at : at + n] = pick(even, n, right, left)
        send_b[at : at + n] = pick(even, n, left, right)


def side_columns(ca, cb, turn):
    turn[...] = jnp.zeros((N, N), F32)
    places = ((0, 4, 0, 124), (4, 4, 8, 4), (8, 4, 16, 12), (12, 2, 24, 22), (14, 2, 32, 30))
    for at, n, low, high in places:
        after, before = both_ways(ca[at : at + n], cb[at : at + n], "gx")
        turn[low : low + n] = after
        turn[high : high + n] = before
    mixed = turn[...].T
    turn[...] = jnp.zeros((N, N), F32)
    after, before = both_ways(ca[16:20], cb[16:20], "gx")
    turn[0:4] = after
    turn[N - 4 : N] = before
    turn[...] = turn[...].T
    return mixed


def outer(x, fill=0.0):
    lane = lanes(x.shape[0])
    return jnp.where((lane < 2) | (lane >= N - 2), x, fill)


def side_field(mixed, slot):
    lane = lanes(N)
    moved = mixed if slot == 0 else pltpu.roll(mixed, N - 8 * slot, 1)
    return jnp.where((lane < 4) | (lane >= 124), moved, 0.0)


def root_viscosity(su, sv, st, sh):
    for at in range(TOP - 8, TOP + N + 8, 8):
        here = slice(at, at + 8)
        up, down = slice(at + 1, at + 9), slice(at - 1, at + 7)
        ue, uw = east(su[0, here], su[1, here]), west(su[0, here], su[1, here])
        ve, vw = east(sv[0, here], sv[1, here]), west(sv[0, here], sv[1, here])
        for t in (0, 1):
            strain_xx = 0.5 * (ue[t] - uw[t])
            strain_yy = 0.5 * (sv[t, up] - sv[t, down])
            shear = 0.25 * (su[t, up] - su[t, down] + (ve[t] - vw[t]))
            delta2 = (
                1.25 * (strain_xx * strain_xx + strain_yy * strain_yy)
                + shear * shear
                + 1.5 * strain_xx * strain_yy
            )
            sh[t, here] = jnp.sqrt(st[t, here] / (2.0 * jnp.sqrt(delta2 + DELTA_MIN * DELTA_MIN)))


def systems(su, sv, st, sh, wx, wy, live, tiles, put_u, put_v):
    for at in range(TOP, TOP + N, 8):
        here = slice(at, at + 8)
        up, down = slice(at + 1, at + 9), slice(at - 1, at + 7)
        cell = slice(at - TOP, at - TOP + 8)
        he, hw = east(sh[0, here], sh[1, here]), west(sh[0, here], sh[1, here])
        ve, vw = east(sv[0, here], sv[1, here]), west(sv[0, here], sv[1, here])
        te, tw = east(st[0, here], st[1, here]), west(st[0, here], st[1, here])
        for t in tiles:
            h, thick = sh[t, here], st[t, here]
            e_edge, w_edge = h * he[t], h * hw[t]
            n_edge, s_edge = h * sh[t, up], h * sh[t, down]
            mass = WEAK * thick
            alive = live(t, cell) > 0.5
            if t == 0:
                extra = mass + WEAK * (n_edge + s_edge)
                right = (
                    mass * su[0, here]
                    + DRIVE * wx(cell)
                    + CORIOLIS * mass * sv[0, here]
                    + WEAK * (n_edge * su[0, up] + s_edge * su[0, down])
                    - 0.5 * PRESS * (te[0] - tw[0])
                )
                scale = 1.0 / (extra + e_edge + w_edge)
                put_u(
                    cell,
                    jnp.where(alive, w_edge * scale, 0.0),
                    jnp.where(alive, e_edge * scale, 0.0),
                    jnp.where(alive, extra * scale, 1.0),
                    jnp.where(alive, right * scale, 0.0),
                )
            extra = mass + WEAK * (e_edge + w_edge)
            right = (
                mass * sv[t, here]
                + DRIVE * wy(t, cell)
                + WEAK * (e_edge * ve[t] + w_edge * vw[t])
                - 0.5 * PRESS * (st[t, up] - st[t, down])
            )
            scale = 1.0 / jnp.where(alive, extra + n_edge + s_edge, 1.0)
            put_v(
                t,
                cell,
                jnp.where(alive, s_edge * scale, 0.0),
                jnp.where(alive, n_edge * scale, 0.0),
                jnp.where(alive, extra * scale, 1.0),
                jnp.where(alive, right * scale, 0.0),
                jnp.where(alive, CORIOLIS * mass * scale, 0.0),
            )


def set_rims(bands):
    one, zero = jnp.ones((8, N), F32), jnp.zeros((8, N), F32)
    for half in (0, 1):
        for k in range(4):
            bands[half, k, 0:8] = one if k == 0 else zero
            bands[half, k, 8 + N : 16 + N] = one if k == 1 else zero


def set_band(bands, k, at, value):
    if at + value.shape[0] == N:
        own = sublanes(value.shape[0]) == value.shape[0] - 1
        value = jnp.where(own, 1.0 if k == 1 else 0.0, value)
    bands[0, k, 8 + at : 8 + at + value.shape[0]] = value


def reduce_piece(bands, last, out):
    half, s = 0, 1
    while s < N:
        final = 2 * s >= N
        for at in range(0, N, 8):
            here = slice(8 + at, 16 + at)
            l, u, e, r = (bands[half, k, here] for k in range(4))
            ll, uu, ee, rr = l, u, e, r
            if s < 8 or at >= s:
                low = slice(8 + at - s, 16 + at - s)
                ll = l * bands[half, 0, low]
                ee = ee + l * bands[half, 2, low]
                rr = rr + l * bands[half, 3, low]
            if s < 8 or at + s < N:
                high = slice(8 + at + s, 16 + at + s)
                uu = u * bands[half, 1, high]
                ee = ee + u * bands[half, 2, high]
                rr = rr + u * bands[half, 3, high]
            q = 1.0 / (ll + uu + ee)
            for k, x in enumerate((ll, uu, ee, rr)):
                if final:
                    out(k, at, x * q)
                if not final or at in (0, N - 8):
                    bands[1 - half, k, here] = x * q
        half, s = 1 - half, 2 * s
    row = lambda k, i: bands[half, k, 8 + i : 9 + i]
    lo, uo, eo, ro = last
    lq, uq, eq, rq = (row(k, N - 2) for k in range(4))
    q = 1.0 / (uo + eo + lo * (lq + eq))
    coupling = [row(k, 0) for k in range(4)]
    coupling += [lo * lq * q, uo * q, (eo + lo * eq) * q, (ro + lo * rq) * q]
    second = [row(k, 1) for k in (0, 1, 3)]
    return coupling, second, [lq, uq, rq]


def solve_pieces(take, me, rowed, extra=None):
    fl, fu, fe, fr, zl, zu, ze, zr = (take(k) for k in range(8))
    nxt = lambda a: pltpu.roll(a, K - 1, 0)
    fl, fu, fe, fr = nxt(fl), nxt(fu), nxt(fe), nxt(fr)
    uu, ee, rr = zu * fu, ze + zu * fe, zr + zu * fr
    q = 1.0 / (zl + ee + uu)
    l, u, e, r = zl * q, uu * q, ee * q, rr * q
    s = 1
    while s < K:
        low = lambda a: pltpu.roll(a, s, 0)
        high = lambda a: pltpu.roll(a, K - s, 0)
        ee = e + l * low(e) + u * high(e)
        rr = r + l * low(r) + u * high(r)
        ll, uu = l * low(l), u * high(u)
        q = 1.0 / (ll + uu + ee)
        l, u, e, r = ll * q, uu * q, ee * q, rr * q
        s *= 2
    zero = jnp.zeros((K, N), F32)
    rowed[0:K] = zero
    rowed[K : 2 * K] = r
    rowed[2 * K : 3 * K] = zero
    before, own = rowed[pl.ds(K - 1 + me, 1), :], rowed[pl.ds(K + me, 1), :]
    if extra is None:
        return before, own
    before2, after = rowed[pl.ds(K - 2 + me, 1), :], rowed[pl.ds(K + 1 + me, 1), :]
    rowed[0:K] = jnp.where(sublanes(K) == K - 1, 0.0, fr + fl * r + fu * nxt(r))
    first = rowed[pl.ds(me, 1), :]
    up, down = extra
    second = up(2) + up(0) * own + up(1) * after
    ahead = down(2) + down(0) * before2 + down(1) * before
    return before, own, ahead, first, second


def rows_of(got, width):
    return lambda k: got[pl.ds(k, K, width), :]


def rows_beside(got, width, base, me):
    up = jnp.minimum(me + 1, K - 1) * width + base
    down = jnp.maximum(me - 1, 0) * width + base
    has_up = jnp.broadcast_to(me < K - 1, (1, N))
    has_down = jnp.broadcast_to(me > 0, (1, N))
    return (
        lambda k: jnp.where(has_up, got[pl.ds(up + k, 1), :], 0.0),
        lambda k: jnp.where(has_down, got[pl.ds(down + k, 1), :], 0.0),
    )


def spread(dest, me, common, forward=None, backward=None):
    width = 8 if forward is None else 16
    for d in range(K):
        at = d * width
        dest[at : at + 8] = common
        if forward is not None:
            dest[at + 8 : at + 16] = pick(me < d, 8, forward, backward)


def tile_of(rows, pad):
    for k, row in enumerate(rows):
        pad[k : k + 1] = row
    return pad[...]


def first_u(vel, wind, thick, alive, ra, rb, ca, cb, send, pl_, pu_, pr_, vsys, sth, su, sv, st, sh, turn, tall, bands, pad):
    mixed = side_columns(ca, cb, turn)
    zero = jnp.zeros((TOP, N), F32)
    for k, s in enumerate((su, sv, st)):
        own = vel.at[k] if k < 2 else thick
        for t in (0, 1):
            s[t, 0:TOP] = zero
            s[t, TOP + N :] = zero
            s[t, TOP : TOP + N] = own[...] if t == 0 else side_field(mixed, k)
        above, below = both_ways(ra[2 * k : 2 * k + 2], rb[2 * k : 2 * k + 2], "gy")
        s[0, TOP - 2 : TOP] = below
        s[0, TOP + N : TOP + N + 2] = above
        s[1, TOP - 2 : TOP] = turn[4 * k : 4 * k + 2]
        s[1, TOP + N : TOP + N + 2] = turn[4 * k + 2 : 4 * k + 4]
    tall[0] = side_field(mixed, 3)
    tall[1] = side_field(mixed, 4)
    root_viscosity(su, sv, st, sh)

    def live(t, cell):
        return alive[cell] if t == 0 else tall[1, cell]

    def wy(t, cell):
        return wind[1, cell] if t == 0 else tall[0, cell]

    def put_u(cell, *values):
        for k, x in enumerate(values):
            tall[2 + k, cell] = x

    def put_v(t, cell, *values):
        for k, x in enumerate(values):
            vsys[k, t, cell] = x

    systems(su, sv, st, sh, lambda cell: wind[0, cell], wy, live, (0, 1), put_u, put_v)
    for t in (0, 1):
        sth[t] = st[t]
    last = []
    for k in range(4):
        turned = tall[2 + k].T
        set_band(bands, k, 0, turned)
        last.append(turned[N - 1 :])
    set_rims(bands)
    outs = {0: pl_, 1: pu_, 3: pr_}

    def out(k, at, x):
        if k != 2:
            outs[k][at : at + 8] = x

    main, second, ahead = reduce_piece(bands, last, out)
    me = lax.axis_index("gx")
    common = tile_of(main, pad)
    pad[...] = jnp.zeros((8, N), F32)
    forward = tile_of(ahead, pad)
    backward = tile_of(second, pad)
    spread(send, me, common, forward, backward)


def load_v(bands, vsys, t, speed):
    last = []
    for k in range(4):
        x = vsys[k, t]
        if k == 3:
            x = x - vsys[4, t] * speed
        set_band(bands, k, 0, x)
        last.append(x[N - 1 :])
    set_rims(bands)
    return last


def first_v(got, pl_, pu_, pr_, vsys, send, u_new, vp, turn, bands, pad, rowed):
    me = lax.axis_index("gx")
    before, own, ahead, first, second = solve_pieces(rows_of(got, 16), me, rowed, rows_beside(got, 16, 8, me))
    turn[...] = pr_[...] + pl_[...] * before + pu_[...] * own
    u_new[0] = turn[...].T
    turn[...] = jnp.zeros((N, N), F32)
    turn[0:1] = first
    turn[1:2] = second
    turn[N - 2 : N - 1] = ahead
    turn[N - 1 : N] = before
    u_new[1] = turn[...].T
    for t in (0, 1):
        last = load_v(bands, vsys, t, u_new[t])

        def out(k, at, x):
            if k != 2:
                vp[min(k, 2), t, at : at + 8] = x

        main, second, ahead = reduce_piece(bands, last, out)
        if t == 0:
            common, extras = tile_of(main, pad), (ahead, second)
    packed = jnp.zeros((1, N), F32)
    inward = lambda x, at: pltpu.roll(jnp.where(lanes(1) < 4, pltpu.roll(x, 2, 1), 0.0), at, 1)
    for k, x in enumerate(main):
        packed = packed + (inward(x, 4 * k) if k else jnp.where(lanes(1) < 4, pltpu.roll(x, 2, 1), 0.0))
    pad[...] = jnp.zeros((8, N), F32)
    forward = tile_of(
        [packed + inward(u_new[1, N - 1 : N], 32)] + extras[0] + [u_new[0, N - 2 : N - 1], u_new[0, N - 1 : N]], pad
    )
    backward = tile_of([packed + inward(u_new[1, 0:1], 32)] + extras[1] + [u_new[0, 1:2], u_new[0, 0:1]], pad)
    spread(send, lax.axis_index("gy"), common, forward, backward)


def second_u(got, vp, u_new, sth, wind, alive, send, pl_, pu_, pr_, vsys, su, sv, sh, tall, bands, pad, rowed):
    me = lax.axis_index("gy")
    up, down = rows_beside(got, 16, 8, me)
    coefs = (lambda k: up(1 + k), lambda k: down(1 + k))
    packed = got[pl.ds(8, K, 16), :]
    unpack = lambda k: outer(pltpu.roll(packed, N - 2 - 4 * k, 1), 1.0 if k in (2, 6) else 0.0)
    zero = jnp.zeros((TOP, N), F32)
    for t in (0, 1):
        before, own, ahead, first, second = solve_pieces(rows_of(got, 16) if t == 0 else unpack, me, rowed, coefs)
        for s in (su, sv):
            s[t, 0:TOP] = zero
            s[t, TOP + N :] = zero
        sv[t, TOP : TOP + N] = vp[2, t] + vp[0, t] * before + vp[1, t] * own
        sv[t, TOP - 1 : TOP] = before
        sv[t, TOP + N : TOP + N + 1] = first
        su[t, TOP : TOP + N] = u_new[t]
        if t == 0:
            sv[0, TOP - 2 : TOP - 1] = ahead
            sv[0, TOP + N + 1 : TOP + N + 2] = second
            su[0, TOP - 2 : TOP - 1] = down(4)
            su[0, TOP - 1 : TOP] = down(5)
            su[0, TOP + N : TOP + N + 1] = up(5)
            su[0, TOP + N + 1 : TOP + N + 2] = up(4)
        else:
            su[1, TOP - 1 : TOP] = outer(pltpu.roll(down(0), N - 34, 1))
            su[1, TOP + N : TOP + N + 1] = outer(pltpu.roll(up(0), N - 34, 1))
    root_viscosity(su, sv, sth, sh)

    def live(t, cell):
        return alive[cell]

    def put_u(cell, *values):
        for k, x in enumerate(values):
            tall[k, cell] = x

    def put_v(t, cell, *values):
        for k, x in enumerate(values):
            vsys[k, t, cell] = x

    systems(su, sv, sth, sh, lambda cell: wind[0, cell], lambda t, cell: wind[1, cell], live, (0,), put_u, put_v)
    last = []
    for k in range(4):
        turned = tall[k].T
        set_band(bands, k, 0, turned)
        last.append(turned[N - 1 :])
    set_rims(bands)
    outs = {0: pl_, 1: pu_, 3: pr_}

    def out(k, at, x):
        if k != 2:
            outs[k][at : at + 8] = x

    main, _, _ = reduce_piece(bands, last, out)
    spread(send, lax.axis_index("gx"), tile_of(main, pad))


def second_v(got, pl_, pu_, pr_, vsys, send, u_new, vp, turn, bands, pad, rowed):
    before, own = solve_pieces(rows_of(got, 8), lax.axis_index("gx"), rowed)
    turn[...] = pr_[...] + pl_[...] * before + pu_[...] * own
    u_new[...] = turn[...].T
    last = load_v(bands, vsys, 0, u_new[...])

    def out(k, at, x):
        if k != 2:
            vp[min(k, 2), at : at + 8] = x

    main, _, _ = reduce_piece(bands, last, out)
    spread(send, lax.axis_index("gy"), tile_of(main, pad))


def finish(got, vp, u_new, out, rowed):
    before, own = solve_pieces(rows_of(got, 8), lax.axis_index("gy"), rowed)
    out[0] = u_new[...]
    out[1] = vp[2] + vp[0] * before + vp[1] * own


def call(kernel, outs, scratch, *args, far=False, flops=None):
    vmem = pl.BlockSpec(memory_space=pltpu.VMEM)
    shapes = [jax.ShapeDtypeStruct(s, F32) for s in outs]
    cost = None if flops is None else pl.CostEstimate(flops=flops, bytes_accessed=0, transcendentals=0)
    return pl.pallas_call(
        kernel,
        out_shape=shapes,
        in_specs=[pl.BlockSpec(memory_space=pltpu.HBM) if far else vmem] * len(args),
        out_specs=[vmem] * len(outs),
        scratch_shapes=[pltpu.VMEM(s, F32) if isinstance(s, tuple) else s for s in scratch],
        compiler_params=pltpu.CompilerParams(vmem_limit_bytes=8 * 1024 * 1024),
        cost_estimate=cost,
    )(*args)


def neighbours(a, b, axis):
    inner = [(i, i ^ 1) for i in range(K)]
    outer = [p for i in range(1, K - 1, 2) for p in ((i, i + 1), (i + 1, i))]
    return lax.ppermute(a, axis, inner), lax.ppermute(b, axis, outer)


def share(rows, axis):
    width = rows.shape[0] // K
    moved = lax.all_to_all(rows.reshape(K, width, N), axis, 0, 0, tiled=True)
    return moved.reshape(K * width, N)


def on_device(velocity, wind, thick, ice, land):
    square, halves, rim = (N, N), (2, N, N), (2, ROWS, N)
    bands, pad, rowed = (2, 4, N + 16, N), (8, N), (3 * K, N)
    flags = pltpu.VMEM(square, jnp.int32)
    sems = pltpu.SemaphoreType.DMA((6,))
    a, b = call(edge_rows, [(8, N)] * 2, [(3, 8, N)] * 2 + [sems], velocity, thick, far=True)
    ra, rb = neighbours(a, b, "gy")
    vel, wind, thick, alive, edges = call(
        load,
        [halves, halves, square, square, (32, N)],
        [flags, flags, square, sems],
        velocity, wind, thick, ice, land,
        far=True, flops=10**8,
    )
    a, b = call(pack_columns, [(24, N)] * 2, [square], edges, ra, rb)
    ca, cb = neighbours(a, b, "gx")
    send, l, u, r, vsys, sth = call(
        first_u,
        [(K * 16, N), square, square, square, (5,) + halves, rim],
        [rim] * 4 + [square, (6, N, N), bands, pad],
        vel, wind, thick, alive, ra, rb, ca, cb,
    )
    got = share(send, "gx")
    send, u_new, vp = call(
        first_v,
        [(K * 16, N), halves, (3,) + halves],
        [square, bands, pad, rowed],
        got, l, u, r, vsys,
    )
    got = share(send, "gy")
    send, l, u, r, vsys = call(
        second_u,
        [(K * 8, N), square, square, square, (5, 1, N, N)],
        [rim] * 3 + [(4, N, N), bands, pad, rowed],
        got, vp, u_new, sth, wind, alive,
    )
    got = share(send, "gx")
    send, u_new, vp = call(
        second_v,
        [(K * 8, N), square, (3, N, N)],
        [square, bands, pad, rowed],
        got, l, u, r, vsys,
    )
    got = share(send, "gy")
    (out,) = call(finish, [halves], [rowed], got, vp, u_new)
    return out


def solution(mesh):
    field = P(None, "gy", "gx")
    flat = P("gy", "gx")
    return jax.shard_map(
        on_device,
        mesh=mesh,
        in_specs=(field, field, flat, flat, flat),
        out_specs=field,
        check_vma=False,
    )
```

```python
import jax
import jax.numpy as jnp
from jax import lax
from jax.experimental import pallas as pl
from jax.experimental.pallas import tpu as pltpu
from jax.sharding import PartitionSpec as P


CORIOLIS = 1.0
DELTA_MIN = 0.25
WIND_GAIN = 0.2

N = 128
K = 16
TOP = 16
ROWS = N + 2 * TOP
CELLS = float(N * N)
WEAK = 1.0 / (16.0 * CELLS)
PRESS = CELLS ** (-0.25)
DRIVE = WIND_GAIN * CELLS ** (-0.75)
F32 = jnp.float32


def lanes(rows):
    return lax.broadcasted_iota(jnp.int32, (rows, N), 1)


def sublanes(rows):
    return lax.broadcasted_iota(jnp.int32, (rows, N), 0)


def east(own, side):
    a, b = pltpu.roll(own, N - 1, 1), pltpu.roll(side, N - 1, 1)
    last = lanes(own.shape[0]) == N - 1
    return jnp.where(last, b, a), jnp.where(last, a, b)


def west(own, side):
    a, b = pltpu.roll(own, 1, 1), pltpu.roll(side, 1, 1)
    first = lanes(own.shape[0]) == 0
    return jnp.where(first, b, a), jnp.where(first, a, b)


def pick(flag, rows, a, b):
    return jnp.where(jnp.broadcast_to(flag, (rows, N)), a, b)


def edge_rows(vel, thick_low, thick_high, send_a, send_b):
    even = lax.rem(lax.axis_index("gy"), 2) == 0
    for k in range(3):
        first = vel[k, 0:2] if k < 2 else thick_low[...]
        final = vel[k, N - 2 : N] if k < 2 else thick_high[...]
        send_a[2 * k : 2 * k + 2] = pick(even, 2, final, first)
        send_b[2 * k : 2 * k + 2] = pick(even, 2, first, final)
    send_a[6:8] = jnp.zeros((2, N), F32)
    send_b[6:8] = jnp.zeros((2, N), F32)


def edge_columns(vel, wind, thick, alive, edges, turn):
    lane = lanes(N)
    mixed = jnp.where(lane < 36, pltpu.roll(alive[...], 32, 1), vel[0])
    mixed = jnp.where(lane < 28, pltpu.roll(wind[1], 24, 1), mixed)
    mixed = jnp.where(lane < 20, pltpu.roll(thick[...], 16, 1), mixed)
    mixed = jnp.where(lane < 12, pltpu.roll(vel[1], 8, 1), mixed)
    mixed = jnp.where(lane < 4, vel[0], mixed)
    turn[...] = mixed.T
    left = ((0, 4), (8, 4), (16, 4), (24, 2), (32, 2))
    right = ((124, 4), (4, 4), (12, 4), (22, 2), (30, 2))
    for base, places in ((0, left), (16, right)):
        for at, n in places:
            edges[base : base + n] = turn[at : at + n]
            base += n


def both_ways(a, b, axis):
    even = lax.rem(lax.axis_index(axis), 2) == 0
    n = a.shape[0]
    return pick(even, n, a, b), pick(even, n, b, a)


def pack_columns(edges, ra, rb, send_a, send_b, turn):
    turn[...] = jnp.zeros((N, N), F32)
    for k in range(3):
        above, below = both_ways(ra[2 * k : 2 * k + 2], rb[2 * k : 2 * k + 2], "gy")
        turn[4 * k : 4 * k + 2] = below
        turn[4 * k + 2 : 4 * k + 4] = above
    turn[...] = turn[...].T
    even = lax.rem(lax.axis_index("gx"), 2) == 0
    for at, n, left, right in (
        (0, 16, edges[0:16], edges[16:32]),
        (16, 4, turn[0:4], turn[N - 4 : N]),
        (20, 4, jnp.zeros((4, N), F32), jnp.zeros((4, N), F32)),
    ):
        send_a[at : at + n] = pick(even, n, right, left)
        send_b[at : at + n] = pick(even, n, left, right)


def side_columns(ca, cb, turn):
    turn[...] = jnp.zeros((N, N), F32)
    places = ((0, 4, 0, 124), (4, 4, 8, 4), (8, 4, 16, 12), (12, 2, 24, 22), (14, 2, 32, 30))
    for at, n, low, high in places:
        after, before = both_ways(ca[at : at + n], cb[at : at + n], "gx")
        turn[low : low + n] = after
        turn[high : high + n] = before
    mixed = turn[...].T
    turn[...] = jnp.zeros((N, N), F32)
    after, before = both_ways(ca[16:20], cb[16:20], "gx")
    turn[0:4] = after
    turn[N - 4 : N] = before
    turn[...] = turn[...].T
    return mixed


def outer(x, fill=0.0):
    lane = lanes(x.shape[0])
    return jnp.where((lane < 2) | (lane >= N - 2), x, fill)


def side_field(mixed, slot):
    lane = lanes(N)
    moved = mixed if slot == 0 else pltpu.roll(mixed, N - 8 * slot, 1)
    return jnp.where((lane < 4) | (lane >= 124), moved, 0.0)


def root_viscosity(su, sv, st, sh):
    for at in range(TOP - 8, TOP + N + 8, 8):
        here = slice(at, at + 8)
        up, down = slice(at + 1, at + 9), slice(at - 1, at + 7)
        ue, uw = east(su[0, here], su[1, here]), west(su[0, here], su[1, here])
        ve, vw = east(sv[0, here], sv[1, here]), west(sv[0, here], sv[1, here])
        for t in (0, 1):
            strain_xx = 0.5 * (ue[t] - uw[t])
            strain_yy = 0.5 * (sv[t, up] - sv[t, down])
            shear = 0.25 * (su[t, up] - su[t, down] + (ve[t] - vw[t]))
            delta2 = (
                1.25 * (strain_xx * strain_xx + strain_yy * strain_yy)
                + shear * shear
                + 1.5 * strain_xx * strain_yy
            )
            sh[t, here] = jnp.sqrt(st[t, here] / (2.0 * jnp.sqrt(delta2 + DELTA_MIN * DELTA_MIN)))


def systems(su, sv, st, sh, wx, wy, live, tiles, put_u, put_v):
    for at in range(TOP, TOP + N, 8):
        here = slice(at, at + 8)
        up, down = slice(at + 1, at + 9), slice(at - 1, at + 7)
        cell = slice(at - TOP, at - TOP + 8)
        he, hw = east(sh[0, here], sh[1, here]), west(sh[0, here], sh[1, here])
        ve, vw = east(sv[0, here], sv[1, here]), west(sv[0, here], sv[1, here])
        te, tw = east(st[0, here], st[1, here]), west(st[0, here], st[1, here])
        for t in tiles:
            h, thick = sh[t, here], st[t, here]
            e_edge, w_edge = h * he[t], h * hw[t]
            n_edge, s_edge = h * sh[t, up], h * sh[t, down]
            mass = WEAK * thick
            alive = live(t, cell) > 0.5
            if t == 0:
                extra = mass + WEAK * (n_edge + s_edge)
                right = (
                    mass * su[0, here]
                    + DRIVE * wx(cell)
                    + CORIOLIS * mass * sv[0, here]
                    + WEAK * (n_edge * su[0, up] + s_edge * su[0, down])
                    - 0.5 * PRESS * (te[0] - tw[0])
                )
                scale = 1.0 / (extra + e_edge + w_edge)
                put_u(
                    cell,
                    jnp.where(alive, w_edge * scale, 0.0),
                    jnp.where(alive, e_edge * scale, 0.0),
                    jnp.where(alive, extra * scale, 1.0),
                    jnp.where(alive, right * scale, 0.0),
                )
            extra = mass + WEAK * (e_edge + w_edge)
            right = (
                mass * sv[t, here]
                + DRIVE * wy(t, cell)
                + WEAK * (e_edge * ve[t] + w_edge * vw[t])
                - 0.5 * PRESS * (st[t, up] - st[t, down])
            )
            scale = 1.0 / jnp.where(alive, extra + n_edge + s_edge, 1.0)
            put_v(
                t,
                cell,
                jnp.where(alive, s_edge * scale, 0.0),
                jnp.where(alive, n_edge * scale, 0.0),
                jnp.where(alive, extra * scale, 1.0),
                jnp.where(alive, right * scale, 0.0),
                jnp.where(alive, CORIOLIS * mass * scale, 0.0),
            )


def set_rims(bands):
    one, zero = jnp.ones((8, N), F32), jnp.zeros((8, N), F32)
    for half in (0, 1):
        for k in range(4):
            bands[half, k, 0:8] = one if k == 0 else zero
            bands[half, k, 8 + N : 16 + N] = one if k == 1 else zero


def set_band(bands, k, at, value):
    if at + value.shape[0] == N:
        own = sublanes(value.shape[0]) == value.shape[0] - 1
        value = jnp.where(own, 1.0 if k == 1 else 0.0, value)
    bands[0, k, 8 + at : 8 + at + value.shape[0]] = value


def reduce_piece(bands, last, out):
    half, s = 0, 1
    while s < N:
        final = 2 * s >= N
        for at in range(0, N, 8):
            here = slice(8 + at, 16 + at)
            l, u, e, r = (bands[half, k, here] for k in range(4))
            ll, uu, ee, rr = l, u, e, r
            if s < 8 or at >= s:
                low = slice(8 + at - s, 16 + at - s)
                ll = l * bands[half, 0, low]
                ee = ee + l * bands[half, 2, low]
                rr = rr + l * bands[half, 3, low]
            if s < 8 or at + s < N:
                high = slice(8 + at + s, 16 + at + s)
                uu = u * bands[half, 1, high]
                ee = ee + u * bands[half, 2, high]
                rr = rr + u * bands[half, 3, high]
            q = 1.0 / (ll + uu + ee)
            for k, x in enumerate((ll, uu, ee, rr)):
                if final:
                    out(k, at, x * q)
                if not final or at in (0, N - 8):
                    bands[1 - half, k, here] = x * q
        half, s = 1 - half, 2 * s
    row = lambda k, i: bands[half, k, 8 + i : 9 + i]
    lo, uo, eo, ro = last
    lq, uq, eq, rq = (row(k, N - 2) for k in range(4))
    q = 1.0 / (uo + eo + lo * (lq + eq))
    coupling = [row(k, 0) for k in range(4)]
    coupling += [lo * lq * q, uo * q, (eo + lo * eq) * q, (ro + lo * rq) * q]
    second = [row(k, 1) for k in (0, 1, 3)]
    return coupling, second, [lq, uq, rq]


def solve_pieces(take, me, rowed, extra=None):
    fl, fu, fe, fr, zl, zu, ze, zr = (take(k) for k in range(8))
    nxt = lambda a: pltpu.roll(a, K - 1, 0)
    fl, fu, fe, fr = nxt(fl), nxt(fu), nxt(fe), nxt(fr)
    uu, ee, rr = zu * fu, ze + zu * fe, zr + zu * fr
    q = 1.0 / (zl + ee + uu)
    l, u, e, r = zl * q, uu * q, ee * q, rr * q
    s = 1
    while s < K:
        low = lambda a: pltpu.roll(a, s, 0)
        high = lambda a: pltpu.roll(a, K - s, 0)
        ee = e + l * low(e) + u * high(e)
        rr = r + l * low(r) + u * high(r)
        ll, uu = l * low(l), u * high(u)
        q = 1.0 / (ll + uu + ee)
        l, u, e, r = ll * q, uu * q, ee * q, rr * q
        s *= 2
    zero = jnp.zeros((K, N), F32)
    rowed[0:K] = zero
    rowed[K : 2 * K] = r
    rowed[2 * K : 3 * K] = zero
    before, own = rowed[pl.ds(K - 1 + me, 1), :], rowed[pl.ds(K + me, 1), :]
    if extra is None:
        return before, own
    before2, after = rowed[pl.ds(K - 2 + me, 1), :], rowed[pl.ds(K + 1 + me, 1), :]
    rowed[0:K] = jnp.where(sublanes(K) == K - 1, 0.0, fr + fl * r + fu * nxt(r))
    first = rowed[pl.ds(me, 1), :]
    up, down = extra
    second = up(2) + up(0) * own + up(1) * after
    ahead = down(2) + down(0) * before2 + down(1) * before
    return before, own, ahead, first, second


def rows_of(got, width):
    return lambda k: got[pl.ds(k, K, width), :]


def rows_beside(got, width, base, me):
    up = jnp.minimum(me + 1, K - 1) * width + base
    down = jnp.maximum(me - 1, 0) * width + base
    has_up = jnp.broadcast_to(me < K - 1, (1, N))
    has_down = jnp.broadcast_to(me > 0, (1, N))
    return (
        lambda k: jnp.where(has_up, got[pl.ds(up + k, 1), :], 0.0),
        lambda k: jnp.where(has_down, got[pl.ds(down + k, 1), :], 0.0),
    )


def spread(dest, me, common, forward=None, backward=None):
    width = 8 if forward is None else 16
    for d in range(K):
        at = d * width
        dest[at : at + 8] = common
        if forward is not None:
            dest[at + 8 : at + 16] = pick(me < d, 8, forward, backward)


def tile_of(rows, pad):
    for k, row in enumerate(rows):
        pad[k : k + 1] = row
    return pad[...]


def first_u(vel, wind, thick, alive, ra, rb, ca, cb, send, pl_, pu_, pr_, vsys, sth, su, sv, st, sh, turn, tall, bands, pad):
    mixed = side_columns(ca, cb, turn)
    zero = jnp.zeros((TOP, N), F32)
    for k, s in enumerate((su, sv, st)):
        own = vel.at[k] if k < 2 else thick
        for t in (0, 1):
            s[t, 0:TOP] = zero
            s[t, TOP + N :] = zero
            s[t, TOP : TOP + N] = own[...] if t == 0 else side_field(mixed, k)
        above, below = both_ways(ra[2 * k : 2 * k + 2], rb[2 * k : 2 * k + 2], "gy")
        s[0, TOP - 2 : TOP] = below
        s[0, TOP + N : TOP + N + 2] = above
        s[1, TOP - 2 : TOP] = turn[4 * k : 4 * k + 2]
        s[1, TOP + N : TOP + N + 2] = turn[4 * k + 2 : 4 * k + 4]
    tall[0] = side_field(mixed, 3)
    tall[1] = side_field(mixed, 4)
    root_viscosity(su, sv, st, sh)

    def live(t, cell):
        return alive[cell] if t == 0 else tall[1, cell]

    def wy(t, cell):
        return wind[1, cell] if t == 0 else tall[0, cell]

    def put_u(cell, *values):
        for k, x in enumerate(values):
            tall[2 + k, cell] = x

    def put_v(t, cell, *values):
        for k, x in enumerate(values):
            vsys[k, t, cell] = x

    systems(su, sv, st, sh, lambda cell: wind[0, cell], wy, live, (0, 1), put_u, put_v)
    for t in (0, 1):
        sth[t] = st[t]
    last = []
    for k in range(4):
        turned = tall[2 + k].T
        set_band(bands, k, 0, turned)
        last.append(turned[N - 1 :])
    set_rims(bands)
    outs = {0: pl_, 1: pu_, 3: pr_}

    def out(k, at, x):
        if k != 2:
            outs[k][at : at + 8] = x

    main, second, ahead = reduce_piece(bands, last, out)
    me = lax.axis_index("gx")
    common = tile_of(main, pad)
    pad[...] = jnp.zeros((8, N), F32)
    forward = tile_of(ahead, pad)
    backward = tile_of(second, pad)
    spread(send, me, common, forward, backward)


def load_v(bands, vsys, t, speed):
    last = []
    for k in range(4):
        x = vsys[k, t]
        if k == 3:
            x = x - vsys[4, t] * speed
        set_band(bands, k, 0, x)
        last.append(x[N - 1 :])
    set_rims(bands)
    return last


def first_v(got, pl_, pu_, pr_, vsys, send, u_new, vp, turn, bands, pad, rowed):
    me = lax.axis_index("gx")
    before, own, ahead, first, second = solve_pieces(rows_of(got, 16), me, rowed, rows_beside(got, 16, 8, me))
    turn[...] = pr_[...] + pl_[...] * before + pu_[...] * own
    u_new[0] = turn[...].T
    turn[...] = jnp.zeros((N, N), F32)
    turn[0:1] = first
    turn[1:2] = second
    turn[N - 2 : N - 1] = ahead
    turn[N - 1 : N] = before
    u_new[1] = turn[...].T
    for t in (0, 1):
        last = load_v(bands, vsys, t, u_new[t])

        def out(k, at, x):
            if k != 2:
                vp[min(k, 2), t, at : at + 8] = x

        main, second, ahead = reduce_piece(bands, last, out)
        if t == 0:
            common, extras = tile_of(main, pad), (ahead, second)
    packed = jnp.zeros((1, N), F32)
    inward = lambda x, at: pltpu.roll(jnp.where(lanes(1) < 4, pltpu.roll(x, 2, 1), 0.0), at, 1)
    for k, x in enumerate(main):
        packed = packed + (inward(x, 4 * k) if k else jnp.where(lanes(1) < 4, pltpu.roll(x, 2, 1), 0.0))
    pad[...] = jnp.zeros((8, N), F32)
    forward = tile_of(
        [packed + inward(u_new[1, N - 1 : N], 32)] + extras[0] + [u_new[0, N - 2 : N - 1], u_new[0, N - 1 : N]], pad
    )
    backward = tile_of([packed + inward(u_new[1, 0:1], 32)] + extras[1] + [u_new[0, 1:2], u_new[0, 0:1]], pad)
    spread(send, lax.axis_index("gy"), common, forward, backward)


def second_u(got, vp, u_new, sth, wind, alive, send, pl_, pu_, pr_, vsys, su, sv, sh, tall, bands, pad, rowed):
    me = lax.axis_index("gy")
    up, down = rows_beside(got, 16, 8, me)
    coefs = (lambda k: up(1 + k), lambda k: down(1 + k))
    packed = got[pl.ds(8, K, 16), :]
    unpack = lambda k: outer(pltpu.roll(packed, N - 2 - 4 * k, 1), 1.0 if k in (2, 6) else 0.0)
    zero = jnp.zeros((TOP, N), F32)
    for t in (0, 1):
        before, own, ahead, first, second = solve_pieces(rows_of(got, 16) if t == 0 else unpack, me, rowed, coefs)
        for s in (su, sv):
            s[t, 0:TOP] = zero
            s[t, TOP + N :] = zero
        sv[t, TOP : TOP + N] = vp[2, t] + vp[0, t] * before + vp[1, t] * own
        sv[t, TOP - 1 : TOP] = before
        sv[t, TOP + N : TOP + N + 1] = first
        su[t, TOP : TOP + N] = u_new[t]
        if t == 0:
            sv[0, TOP - 2 : TOP - 1] = ahead
            sv[0, TOP + N + 1 : TOP + N + 2] = second
            su[0, TOP - 2 : TOP - 1] = down(4)
            su[0, TOP - 1 : TOP] = down(5)
            su[0, TOP + N : TOP + N + 1] = up(5)
            su[0, TOP + N + 1 : TOP + N + 2] = up(4)
        else:
            su[1, TOP - 1 : TOP] = outer(pltpu.roll(down(0), N - 34, 1))
            su[1, TOP + N : TOP + N + 1] = outer(pltpu.roll(up(0), N - 34, 1))
    root_viscosity(su, sv, sth, sh)

    def live(t, cell):
        return alive[cell]

    def put_u(cell, *values):
        for k, x in enumerate(values):
            tall[k, cell] = x

    def put_v(t, cell, *values):
        for k, x in enumerate(values):
            vsys[k, t, cell] = x

    systems(su, sv, sth, sh, lambda cell: wind[0, cell], lambda t, cell: wind[1, cell], live, (0,), put_u, put_v)
    last = []
    for k in range(4):
        turned = tall[k].T
        set_band(bands, k, 0, turned)
        last.append(turned[N - 1 :])
    set_rims(bands)
    outs = {0: pl_, 1: pu_, 3: pr_}

    def out(k, at, x):
        if k != 2:
            outs[k][at : at + 8] = x

    main, _, _ = reduce_piece(bands, last, out)
    spread(send, lax.axis_index("gx"), tile_of(main, pad))


def second_v(got, pl_, pu_, pr_, vsys, send, u_new, vp, turn, bands, pad, rowed):
    before, own = solve_pieces(rows_of(got, 8), lax.axis_index("gx"), rowed)
    turn[...] = pr_[...] + pl_[...] * before + pu_[...] * own
    u_new[...] = turn[...].T
    last = load_v(bands, vsys, 0, u_new[...])

    def out(k, at, x):
        if k != 2:
            vp[min(k, 2), at : at + 8] = x

    main, _, _ = reduce_piece(bands, last, out)
    spread(send, lax.axis_index("gy"), tile_of(main, pad))


def finish(got, vp, u_new, out, rowed):
    before, own = solve_pieces(rows_of(got, 8), lax.axis_index("gy"), rowed)
    out[0] = u_new[...]
    out[1] = vp[2] + vp[0] * before + vp[1] * own


def call(kernel, outs, scratch, *args, flops=None):
    vmem = pl.BlockSpec(memory_space=pltpu.VMEM)
    shapes = [jax.ShapeDtypeStruct(s, F32) for s in outs]
    cost = None if flops is None else pl.CostEstimate(flops=flops, bytes_accessed=0, transcendentals=0)
    return pl.pallas_call(
        kernel,
        out_shape=shapes,
        in_specs=[vmem] * len(args),
        out_specs=[vmem] * len(outs),
        scratch_shapes=[pltpu.VMEM(s, F32) for s in scratch],
        compiler_params=pltpu.CompilerParams(vmem_limit_bytes=8 * 1024 * 1024),
        cost_estimate=cost,
    )(*args)


def neighbours(a, b, axis):
    inner = [(i, i ^ 1) for i in range(K)]
    outer = [p for i in range(1, K - 1, 2) for p in ((i, i + 1), (i + 1, i))]
    far = lax.ppermute(b, axis, outer)
    near = lax.ppermute(a, axis, inner)
    return near, far


def share(rows, axis):
    width = rows.shape[0] // K
    moved = lax.all_to_all(rows.reshape(K, width, N), axis, 0, 0, tiled=True)
    return moved.reshape(K * width, N)


def on_device(vel, wind, thick, ice, land):
    square, halves, rim = (N, N), (2, N, N), (2, ROWS, N)
    bands, pad, rowed = (2, 4, N + 16, N), (8, N), (3 * K, N)
    a, b = call(edge_rows, [(8, N)] * 2, [], vel, thick[:2], thick[N - 2 :])
    ra, rb = neighbours(a, b, "gy")
    alive = (ice * (1 - land)).astype(F32)
    (edges,) = call(edge_columns, [(32, N)], [square], vel, wind, thick, alive, flops=10**8)
    a, b = call(pack_columns, [(24, N)] * 2, [square], edges, ra, rb)
    ca, cb = neighbours(a, b, "gx")
    send, l, u, r, vsys, sth = call(
        first_u,
        [(K * 16, N), square, square, square, (5,) + halves, rim],
        [rim] * 4 + [square, (6, N, N), bands, pad],
        vel, wind, thick, alive, ra, rb, ca, cb,
    )
    got = share(send, "gx")
    send, u_new, vp = call(
        first_v,
        [(K * 16, N), halves, (3,) + halves],
        [square, bands, pad, rowed],
        got, l, u, r, vsys,
    )
    got = share(send, "gy")
    send, l, u, r, vsys = call(
        second_u,
        [(K * 8, N), square, square, square, (5, 1, N, N)],
        [rim] * 3 + [(4, N, N), bands, pad, rowed],
        got, vp, u_new, sth, wind, alive,
    )
    got = share(send, "gx")
    send, u_new, vp = call(
        second_v,
        [(K * 8, N), square, (3, N, N)],
        [square, bands, pad, rowed],
        got, l, u, r, vsys,
    )
    got = share(send, "gy")
    (out,) = call(finish, [halves], [rowed], got, vp, u_new)
    return out


def solution(mesh):
    field = P(None, "gy", "gx")
    flat = P("gy", "gx")
    return jax.shard_map(
        on_device,
        mesh=mesh,
        in_specs=(field, field, flat, flat, flat),
        out_specs=field,
        check_vma=False,
    )
```

```python
import jax
import jax.numpy as jnp
from jax import lax
from jax.experimental import pallas as pl
from jax.experimental.pallas import tpu as pltpu
from jax.sharding import PartitionSpec as P


CORIOLIS = 1.0
DELTA_MIN = 0.25
WIND_GAIN = 0.2

N = 128
K = 16
TOP = 16
ROWS = N + 2 * TOP
CELLS = float(N * N)
WEAK = 1.0 / (16.0 * CELLS)
PRESS = CELLS ** (-0.25)
DRIVE = WIND_GAIN * CELLS ** (-0.75)
F32 = jnp.float32


def lanes(rows):
    return lax.broadcasted_iota(jnp.int32, (rows, N), 1)


def sublanes(rows):
    return lax.broadcasted_iota(jnp.int32, (rows, N), 0)


def east(own, side):
    a, b = pltpu.roll(own, N - 1, 1), pltpu.roll(side, N - 1, 1)
    last = lanes(own.shape[0]) == N - 1
    return jnp.where(last, b, a), jnp.where(last, a, b)


def west(own, side):
    a, b = pltpu.roll(own, 1, 1), pltpu.roll(side, 1, 1)
    first = lanes(own.shape[0]) == 0
    return jnp.where(first, b, a), jnp.where(first, a, b)


def pick(flag, rows, a, b):
    return jnp.where(jnp.broadcast_to(flag, (rows, N)), a, b)


def edge_rows(vel, thick):
    even = lax.rem(lax.axis_index("gy"), 2) == 0
    fields = jnp.stack([vel[0], vel[1], thick])
    first, final = fields[:, :2], fields[:, N - 2 :]
    return jnp.where(even, final, first), jnp.where(even, first, final)


def edge_columns(vel, wind, thick, alive, edges, turn):
    lane = lanes(N)
    mixed = jnp.where(lane < 36, pltpu.roll(alive[...], 32, 1), vel[0])
    mixed = jnp.where(lane < 28, pltpu.roll(wind[1], 24, 1), mixed)
    mixed = jnp.where(lane < 20, pltpu.roll(thick[...], 16, 1), mixed)
    mixed = jnp.where(lane < 12, pltpu.roll(vel[1], 8, 1), mixed)
    mixed = jnp.where(lane < 4, vel[0], mixed)
    turn[...] = mixed.T
    left = ((0, 4), (8, 4), (16, 4), (24, 2), (32, 2))
    right = ((124, 4), (4, 4), (12, 4), (22, 2), (30, 2))
    for base, places in ((0, left), (16, right)):
        for at, n in places:
            edges[base : base + n] = turn[at : at + n]
            base += n


def both_ways(a, b, axis):
    even = lax.rem(lax.axis_index(axis), 2) == 0
    n = a.shape[0]
    return pick(even, n, a, b), pick(even, n, b, a)


def pack_columns(edges, ra, rb, send_a, send_b, turn):
    turn[...] = jnp.zeros((N, N), F32)
    for k in range(3):
        above, below = both_ways(ra[k], rb[k], "gy")
        turn[4 * k : 4 * k + 2] = below
        turn[4 * k + 2 : 4 * k + 4] = above
    turn[...] = turn[...].T
    even = lax.rem(lax.axis_index("gx"), 2) == 0
    for at, n, left, right in (
        (0, 16, edges[0:16], edges[16:32]),
        (16, 4, turn[0:4], turn[N - 4 : N]),
        (20, 4, jnp.zeros((4, N), F32), jnp.zeros((4, N), F32)),
    ):
        send_a[at : at + n] = pick(even, n, right, left)
        send_b[at : at + n] = pick(even, n, left, right)


def side_columns(ca, cb, turn):
    turn[...] = jnp.zeros((N, N), F32)
    places = ((0, 4, 0, 124), (4, 4, 8, 4), (8, 4, 16, 12), (12, 2, 24, 22), (14, 2, 32, 30))
    for at, n, low, high in places:
        after, before = both_ways(ca[at : at + n], cb[at : at + n], "gx")
        turn[low : low + n] = after
        turn[high : high + n] = before
    mixed = turn[...].T
    turn[...] = jnp.zeros((N, N), F32)
    after, before = both_ways(ca[16:20], cb[16:20], "gx")
    turn[0:4] = after
    turn[N - 4 : N] = before
    turn[...] = turn[...].T
    return mixed


def outer(x, fill=0.0):
    lane = lanes(x.shape[0])
    return jnp.where((lane < 2) | (lane >= N - 2), x, fill)


def side_field(mixed, slot):
    lane = lanes(N)
    moved = mixed if slot == 0 else pltpu.roll(mixed, N - 8 * slot, 1)
    return jnp.where((lane < 4) | (lane >= 124), moved, 0.0)


def root_viscosity(su, sv, st, sh):
    for at in range(TOP - 8, TOP + N + 8, 8):
        here = slice(at, at + 8)
        up, down = slice(at + 1, at + 9), slice(at - 1, at + 7)
        ue, uw = east(su[0, here], su[1, here]), west(su[0, here], su[1, here])
        ve, vw = east(sv[0, here], sv[1, here]), west(sv[0, here], sv[1, here])
        for t in (0, 1):
            strain_xx = 0.5 * (ue[t] - uw[t])
            strain_yy = 0.5 * (sv[t, up] - sv[t, down])
            shear = 0.25 * (su[t, up] - su[t, down] + (ve[t] - vw[t]))
            delta2 = (
                1.25 * (strain_xx * strain_xx + strain_yy * strain_yy)
                + shear * shear
                + 1.5 * strain_xx * strain_yy
            )
            sh[t, here] = jnp.sqrt(st[t, here] / (2.0 * jnp.sqrt(delta2 + DELTA_MIN * DELTA_MIN)))


def systems(su, sv, st, sh, wx, wy, live, tiles, put_u, put_v):
    for at in range(TOP, TOP + N, 8):
        here = slice(at, at + 8)
        up, down = slice(at + 1, at + 9), slice(at - 1, at + 7)
        cell = slice(at - TOP, at - TOP + 8)
        he, hw = east(sh[0, here], sh[1, here]), west(sh[0, here], sh[1, here])
        ve, vw = east(sv[0, here], sv[1, here]), west(sv[0, here], sv[1, here])
        te, tw = east(st[0, here], st[1, here]), west(st[0, here], st[1, here])
        for t in tiles:
            h, thick = sh[t, here], st[t, here]
            e_edge, w_edge = h * he[t], h * hw[t]
            n_edge, s_edge = h * sh[t, up], h * sh[t, down]
            mass = WEAK * thick
            alive = live(t, cell) > 0.5
            if t == 0:
                extra = mass + WEAK * (n_edge + s_edge)
                right = (
                    mass * su[0, here]
                    + DRIVE * wx(cell)
                    + CORIOLIS * mass * sv[0, here]
                    + WEAK * (n_edge * su[0, up] + s_edge * su[0, down])
                    - 0.5 * PRESS * (te[0] - tw[0])
                )
                scale = 1.0 / (extra + e_edge + w_edge)
                put_u(
                    cell,
                    jnp.where(alive, w_edge * scale, 0.0),
                    jnp.where(alive, e_edge * scale, 0.0),
                    jnp.where(alive, extra * scale, 1.0),
                    jnp.where(alive, right * scale, 0.0),
                )
            extra = mass + WEAK * (e_edge + w_edge)
            right = (
                mass * sv[t, here]
                + DRIVE * wy(t, cell)
                + WEAK * (e_edge * ve[t] + w_edge * vw[t])
                - 0.5 * PRESS * (st[t, up] - st[t, down])
            )
            scale = 1.0 / jnp.where(alive, extra + n_edge + s_edge, 1.0)
            put_v(
                t,
                cell,
                jnp.where(alive, s_edge * scale, 0.0),
                jnp.where(alive, n_edge * scale, 0.0),
                jnp.where(alive, extra * scale, 1.0),
                jnp.where(alive, right * scale, 0.0),
                jnp.where(alive, CORIOLIS * mass * scale, 0.0),
            )


def set_rims(bands):
    one, zero = jnp.ones((8, N), F32), jnp.zeros((8, N), F32)
    for half in (0, 1):
        for k in range(4):
            bands[half, k, 0:8] = one if k == 0 else zero
            bands[half, k, 8 + N : 16 + N] = one if k == 1 else zero


def set_band(bands, k, at, value):
    if at + value.shape[0] == N:
        own = sublanes(value.shape[0]) == value.shape[0] - 1
        value = jnp.where(own, 1.0 if k == 1 else 0.0, value)
    bands[0, k, 8 + at : 8 + at + value.shape[0]] = value


def reduce_piece(bands, last, out):
    half, s = 0, 1
    while s < N:
        final = 2 * s >= N
        for at in range(0, N, 8):
            here = slice(8 + at, 16 + at)
            l, u, e, r = (bands[half, k, here] for k in range(4))
            ll, uu, ee, rr = l, u, e, r
            if s < 8 or at >= s:
                low = slice(8 + at - s, 16 + at - s)
                ll = l * bands[half, 0, low]
                ee = ee + l * bands[half, 2, low]
                rr = rr + l * bands[half, 3, low]
            if s < 8 or at + s < N:
                high = slice(8 + at + s, 16 + at + s)
                uu = u * bands[half, 1, high]
                ee = ee + u * bands[half, 2, high]
                rr = rr + u * bands[half, 3, high]
            q = 1.0 / (ll + uu + ee)
            for k, x in enumerate((ll, uu, ee, rr)):
                if final:
                    out(k, at, x * q)
                if not final or at in (0, N - 8):
                    bands[1 - half, k, here] = x * q
        half, s = 1 - half, 2 * s
    row = lambda k, i: bands[half, k, 8 + i : 9 + i]
    lo, uo, eo, ro = last
    lq, uq, eq, rq = (row(k, N - 2) for k in range(4))
    q = 1.0 / (uo + eo + lo * (lq + eq))
    coupling = [row(k, 0) for k in range(4)]
    coupling += [lo * lq * q, uo * q, (eo + lo * eq) * q, (ro + lo * rq) * q]
    second = [row(k, 1) for k in (0, 1, 3)]
    return coupling, second, [lq, uq, rq]


def solve_pieces(take, me, rowed, extra=None):
    fl, fu, fe, fr, zl, zu, ze, zr = (take(k) for k in range(8))
    nxt = lambda a: pltpu.roll(a, K - 1, 0)
    fl, fu, fe, fr = nxt(fl), nxt(fu), nxt(fe), nxt(fr)
    uu, ee, rr = zu * fu, ze + zu * fe, zr + zu * fr
    q = 1.0 / (zl + ee + uu)
    l, u, e, r = zl * q, uu * q, ee * q, rr * q
    s = 1
    while s < K:
        low = lambda a: pltpu.roll(a, s, 0)
        high = lambda a: pltpu.roll(a, K - s, 0)
        ee = e + l * low(e) + u * high(e)
        rr = r + l * low(r) + u * high(r)
        ll, uu = l * low(l), u * high(u)
        q = 1.0 / (ll + uu + ee)
        l, u, e, r = ll * q, uu * q, ee * q, rr * q
        s *= 2
    zero = jnp.zeros((K, N), F32)
    rowed[0:K] = zero
    rowed[K : 2 * K] = r
    rowed[2 * K : 3 * K] = zero
    before, own = rowed[pl.ds(K - 1 + me, 1), :], rowed[pl.ds(K + me, 1), :]
    if extra is None:
        return before, own
    before2, after = rowed[pl.ds(K - 2 + me, 1), :], rowed[pl.ds(K + 1 + me, 1), :]
    rowed[0:K] = jnp.where(sublanes(K) == K - 1, 0.0, fr + fl * r + fu * nxt(r))
    first = rowed[pl.ds(me, 1), :]
    up, down = extra
    second = up(2) + up(0) * own + up(1) * after
    ahead = down(2) + down(0) * before2 + down(1) * before
    return before, own, ahead, first, second


def rows_of(got, width):
    return lambda k: got[pl.ds(k, K, width), :]


def rows_beside(got, width, base, me):
    up = jnp.minimum(me + 1, K - 1) * width + base
    down = jnp.maximum(me - 1, 0) * width + base
    has_up = jnp.broadcast_to(me < K - 1, (1, N))
    has_down = jnp.broadcast_to(me > 0, (1, N))
    return (
        lambda k: jnp.where(has_up, got[pl.ds(up + k, 1), :], 0.0),
        lambda k: jnp.where(has_down, got[pl.ds(down + k, 1), :], 0.0),
    )


def spread(dest, me, common, forward=None, backward=None):
    width = 8 if forward is None else 16
    for d in range(K):
        at = d * width
        dest[at : at + 8] = common
        if forward is not None:
            dest[at + 8 : at + 16] = pick(me < d, 8, forward, backward)


def tile_of(rows, pad):
    for k, row in enumerate(rows):
        pad[k : k + 1] = row
    return pad[...]


def first_u(vel, wind, thick, alive, ra, rb, ca, cb, send, pl_, pu_, pr_, vsys, sth, su, sv, st, sh, turn, tall, bands, pad):
    mixed = side_columns(ca, cb, turn)
    zero = jnp.zeros((TOP, N), F32)
    for k, s in enumerate((su, sv, st)):
        own = vel.at[k] if k < 2 else thick
        for t in (0, 1):
            s[t, 0:TOP] = zero
            s[t, TOP + N :] = zero
            s[t, TOP : TOP + N] = own[...] if t == 0 else side_field(mixed, k)
        above, below = both_ways(ra[k], rb[k], "gy")
        s[0, TOP - 2 : TOP] = below
        s[0, TOP + N : TOP + N + 2] = above
        s[1, TOP - 2 : TOP] = turn[4 * k : 4 * k + 2]
        s[1, TOP + N : TOP + N + 2] = turn[4 * k + 2 : 4 * k + 4]
    tall[0] = side_field(mixed, 3)
    tall[1] = side_field(mixed, 4)
    root_viscosity(su, sv, st, sh)

    def live(t, cell):
        return alive[cell] if t == 0 else tall[1, cell]

    def wy(t, cell):
        return wind[1, cell] if t == 0 else tall[0, cell]

    def put_u(cell, *values):
        for k, x in enumerate(values):
            tall[2 + k, cell] = x

    def put_v(t, cell, *values):
        for k, x in enumerate(values):
            vsys[k, t, cell] = x

    systems(su, sv, st, sh, lambda cell: wind[0, cell], wy, live, (0, 1), put_u, put_v)
    for t in (0, 1):
        sth[t] = st[t]
    last = []
    for k in range(4):
        turned = tall[2 + k].T
        set_band(bands, k, 0, turned)
        last.append(turned[N - 1 :])
    set_rims(bands)
    outs = {0: pl_, 1: pu_, 3: pr_}

    def out(k, at, x):
        if k != 2:
            outs[k][at : at + 8] = x

    main, second, ahead = reduce_piece(bands, last, out)
    me = lax.axis_index("gx")
    common = tile_of(main, pad)
    pad[...] = jnp.zeros((8, N), F32)
    forward = tile_of(ahead, pad)
    backward = tile_of(second, pad)
    spread(send, me, common, forward, backward)


def load_v(bands, vsys, t, speed):
    last = []
    for k in range(4):
        x = vsys[k, t]
        if k == 3:
            x = x - vsys[4, t] * speed
        set_band(bands, k, 0, x)
        last.append(x[N - 1 :])
    set_rims(bands)
    return last


def first_v(got, pl_, pu_, pr_, vsys, send, u_new, vp, turn, bands, pad, rowed):
    me = lax.axis_index("gx")
    before, own, ahead, first, second = solve_pieces(rows_of(got, 16), me, rowed, rows_beside(got, 16, 8, me))
    turn[...] = pr_[...] + pl_[...] * before + pu_[...] * own
    u_new[0] = turn[...].T
    turn[...] = jnp.zeros((N, N), F32)
    turn[0:1] = first
    turn[1:2] = second
    turn[N - 2 : N - 1] = ahead
    turn[N - 1 : N] = before
    u_new[1] = turn[...].T
    for t in (0, 1):
        last = load_v(bands, vsys, t, u_new[t])

        def out(k, at, x):
            if k != 2:
                vp[min(k, 2), t, at : at + 8] = x

        main, second, ahead = reduce_piece(bands, last, out)
        if t == 0:
            common, extras = tile_of(main, pad), (ahead, second)
    packed = jnp.zeros((1, N), F32)
    inward = lambda x, at: pltpu.roll(jnp.where(lanes(1) < 4, pltpu.roll(x, 2, 1), 0.0), at, 1)
    for k, x in enumerate(main):
        packed = packed + (inward(x, 4 * k) if k else jnp.where(lanes(1) < 4, pltpu.roll(x, 2, 1), 0.0))
    pad[...] = jnp.zeros((8, N), F32)
    forward = tile_of(
        [packed + inward(u_new[1, N - 1 : N], 32)] + extras[0] + [u_new[0, N - 2 : N - 1], u_new[0, N - 1 : N]], pad
    )
    backward = tile_of([packed + inward(u_new[1, 0:1], 32)] + extras[1] + [u_new[0, 1:2], u_new[0, 0:1]], pad)
    spread(send, lax.axis_index("gy"), common, forward, backward)


def second_u(got, vp, u_new, sth, wind, alive, send, pl_, pu_, pr_, vsys, su, sv, sh, tall, bands, pad, rowed):
    me = lax.axis_index("gy")
    up, down = rows_beside(got, 16, 8, me)
    coefs = (lambda k: up(1 + k), lambda k: down(1 + k))
    packed = got[pl.ds(8, K, 16), :]
    unpack = lambda k: outer(pltpu.roll(packed, N - 2 - 4 * k, 1), 1.0 if k in (2, 6) else 0.0)
    zero = jnp.zeros((TOP, N), F32)
    for t in (0, 1):
        before, own, ahead, first, second = solve_pieces(rows_of(got, 16) if t == 0 else unpack, me, rowed, coefs)
        for s in (su, sv):
            s[t, 0:TOP] = zero
            s[t, TOP + N :] = zero
        sv[t, TOP : TOP + N] = vp[2, t] + vp[0, t] * before + vp[1, t] * own
        sv[t, TOP - 1 : TOP] = before
        sv[t, TOP + N : TOP + N + 1] = first
        su[t, TOP : TOP + N] = u_new[t]
        if t == 0:
            sv[0, TOP - 2 : TOP - 1] = ahead
            sv[0, TOP + N + 1 : TOP + N + 2] = second
            su[0, TOP - 2 : TOP - 1] = down(4)
            su[0, TOP - 1 : TOP] = down(5)
            su[0, TOP + N : TOP + N + 1] = up(5)
            su[0, TOP + N + 1 : TOP + N + 2] = up(4)
        else:
            su[1, TOP - 1 : TOP] = outer(pltpu.roll(down(0), N - 34, 1))
            su[1, TOP + N : TOP + N + 1] = outer(pltpu.roll(up(0), N - 34, 1))
    root_viscosity(su, sv, sth, sh)

    def live(t, cell):
        return alive[cell]

    def put_u(cell, *values):
        for k, x in enumerate(values):
            tall[k, cell] = x

    def put_v(t, cell, *values):
        for k, x in enumerate(values):
            vsys[k, t, cell] = x

    systems(su, sv, sth, sh, lambda cell: wind[0, cell], lambda t, cell: wind[1, cell], live, (0,), put_u, put_v)
    last = []
    for k in range(4):
        turned = tall[k].T
        set_band(bands, k, 0, turned)
        last.append(turned[N - 1 :])
    set_rims(bands)
    outs = {0: pl_, 1: pu_, 3: pr_}

    def out(k, at, x):
        if k != 2:
            outs[k][at : at + 8] = x

    main, _, _ = reduce_piece(bands, last, out)
    spread(send, lax.axis_index("gx"), tile_of(main, pad))


def second_v(got, pl_, pu_, pr_, vsys, send, u_new, vp, turn, bands, pad, rowed):
    before, own = solve_pieces(rows_of(got, 8), lax.axis_index("gx"), rowed)
    turn[...] = pr_[...] + pl_[...] * before + pu_[...] * own
    u_new[...] = turn[...].T
    last = load_v(bands, vsys, 0, u_new[...])

    def out(k, at, x):
        if k != 2:
            vp[min(k, 2), at : at + 8] = x

    main, _, _ = reduce_piece(bands, last, out)
    spread(send, lax.axis_index("gy"), tile_of(main, pad))


def finish(got, vp, u_new, out, rowed):
    before, own = solve_pieces(rows_of(got, 8), lax.axis_index("gy"), rowed)
    out[0] = u_new[...]
    out[1] = vp[2] + vp[0] * before + vp[1] * own


def call(kernel, outs, scratch, *args, flops=None):
    vmem = pl.BlockSpec(memory_space=pltpu.VMEM)
    shapes = [jax.ShapeDtypeStruct(s, F32) for s in outs]
    cost = None if flops is None else pl.CostEstimate(flops=flops, bytes_accessed=0, transcendentals=0)
    return pl.pallas_call(
        kernel,
        out_shape=shapes,
        in_specs=[vmem] * len(args),
        out_specs=[vmem] * len(outs),
        scratch_shapes=[pltpu.VMEM(s, F32) for s in scratch],
        compiler_params=pltpu.CompilerParams(vmem_limit_bytes=8 * 1024 * 1024),
        cost_estimate=cost,
    )(*args)


def neighbours(a, b, axis):
    inner = [(i, i ^ 1) for i in range(K)]
    outer = [p for i in range(1, K - 1, 2) for p in ((i, i + 1), (i + 1, i))]
    far = lax.ppermute(b, axis, outer)
    near = lax.ppermute(a, axis, inner)
    return near, far


def share(rows, axis):
    width = rows.shape[0] // K
    moved = lax.all_to_all(rows.reshape(K, width, N), axis, 0, 0, tiled=True)
    return moved.reshape(K * width, N)


def on_device(vel, wind, thick, ice, land):
    square, halves, rim = (N, N), (2, N, N), (2, ROWS, N)
    bands, pad, rowed = (2, 4, N + 16, N), (8, N), (3 * K, N)
    a, b = edge_rows(vel, thick)
    ra, rb = neighbours(a, b, "gy")
    alive = (ice * (1 - land)).astype(F32)
    (edges,) = call(edge_columns, [(32, N)], [square], vel, wind, thick, alive, flops=10**8)
    a, b = call(pack_columns, [(24, N)] * 2, [square], edges, ra, rb)
    ca, cb = neighbours(a, b, "gx")
    send, l, u, r, vsys, sth = call(
        first_u,
        [(K * 16, N), square, square, square, (5,) + halves, rim],
        [rim] * 4 + [square, (6, N, N), bands, pad],
        vel, wind, thick, alive, ra, rb, ca, cb,
    )
    got = share(send, "gx")
    send, u_new, vp = call(
        first_v,
        [(K * 16, N), halves, (3,) + halves],
        [square, bands, pad, rowed],
        got, l, u, r, vsys,
    )
    got = share(send, "gy")
    send, l, u, r, vsys = call(
        second_u,
        [(K * 8, N), square, square, square, (5, 1, N, N)],
        [rim] * 3 + [(4, N, N), bands, pad, rowed],
        got, vp, u_new, sth, wind, alive,
    )
    got = share(send, "gx")
    send, u_new, vp = call(
        second_v,
        [(K * 8, N), square, (3, N, N)],
        [square, bands, pad, rowed],
        got, l, u, r, vsys,
    )
    got = share(send, "gy")
    (out,) = call(finish, [halves], [rowed], got, vp, u_new)
    return out


def solution(mesh):
    field = P(None, "gy", "gx")
    flat = P("gy", "gx")
    return jax.shard_map(
        on_device,
        mesh=mesh,
        in_specs=(field, field, flat, flat, flat),
        out_specs=field,
        check_vma=False,
    )
```

```python
import jax
import jax.numpy as jnp
from jax import lax
from jax.experimental import pallas as pl
from jax.experimental.pallas import tpu as pltpu
from jax.sharding import PartitionSpec as P


CORIOLIS = 1.0
DELTA_MIN = 0.25
WIND_GAIN = 0.2

N = 128
K = 16
TOP = 16
ROWS = N + 2 * TOP
CELLS = float(N * N)
WEAK = 1.0 / (16.0 * CELLS)
PRESS = CELLS ** (-0.25)
DRIVE = WIND_GAIN * CELLS ** (-0.75)
F32 = jnp.float32


def lanes(rows):
    return lax.broadcasted_iota(jnp.int32, (rows, N), 1)


def sublanes(rows):
    return lax.broadcasted_iota(jnp.int32, (rows, N), 0)


def east(own, side):
    a, b = pltpu.roll(own, N - 1, 1), pltpu.roll(side, N - 1, 1)
    last = lanes(own.shape[0]) == N - 1
    return jnp.where(last, b, a), jnp.where(last, a, b)


def west(own, side):
    a, b = pltpu.roll(own, 1, 1), pltpu.roll(side, 1, 1)
    first = lanes(own.shape[0]) == 0
    return jnp.where(first, b, a), jnp.where(first, a, b)


def pick(flag, rows, a, b):
    return jnp.where(jnp.broadcast_to(flag, (rows, N)), a, b)


def edge_rows(vel, thick):
    even = lax.rem(lax.axis_index("gy"), 2) == 0
    fields = jnp.stack([vel[0], vel[1], thick])
    first, final = fields[:, :2], fields[:, N - 2 :]
    return jnp.where(even, final, first), jnp.where(even, first, final)


def edge_columns(vel, wind, thick, alive, edges, turn):
    lane = lanes(N)
    mixed = jnp.where(lane < 36, pltpu.roll(alive[...], 32, 1), vel[0])
    mixed = jnp.where(lane < 28, pltpu.roll(wind[1], 24, 1), mixed)
    mixed = jnp.where(lane < 20, pltpu.roll(thick[...], 16, 1), mixed)
    mixed = jnp.where(lane < 12, pltpu.roll(vel[1], 8, 1), mixed)
    mixed = jnp.where(lane < 4, vel[0], mixed)
    turn[...] = mixed.T
    left = ((0, 4), (8, 4), (16, 4), (24, 2), (32, 2))
    right = ((124, 4), (4, 4), (12, 4), (22, 2), (30, 2))
    for base, places in ((0, left), (16, right)):
        for at, n in places:
            edges[base : base + n] = turn[at : at + n]
            base += n


def both_ways(a, b, axis):
    even = lax.rem(lax.axis_index(axis), 2) == 0
    n = a.shape[0]
    return pick(even, n, a, b), pick(even, n, b, a)


def pack_columns(edges, ra, rb, send_a, send_b, turn):
    turn[...] = jnp.zeros((N, N), F32)
    for k in range(3):
        above, below = both_ways(ra[k], rb[k], "gy")
        turn[4 * k : 4 * k + 2] = below
        turn[4 * k + 2 : 4 * k + 4] = above
    turn[...] = turn[...].T
    even = lax.rem(lax.axis_index("gx"), 2) == 0
    for at, n, left, right in (
        (0, 16, edges[0:16], edges[16:32]),
        (16, 4, turn[0:4], turn[N - 4 : N]),
        (20, 4, jnp.zeros((4, N), F32), jnp.zeros((4, N), F32)),
    ):
        send_a[at : at + n] = pick(even, n, right, left)
        send_b[at : at + n] = pick(even, n, left, right)


def side_columns(ca, cb, turn):
    turn[...] = jnp.zeros((N, N), F32)
    places = ((0, 4, 0, 124), (4, 4, 8, 4), (8, 4, 16, 12), (12, 2, 24, 22), (14, 2, 32, 30))
    for at, n, low, high in places:
        after, before = both_ways(ca[at : at + n], cb[at : at + n], "gx")
        turn[low : low + n] = after
        turn[high : high + n] = before
    mixed = turn[...].T
    turn[...] = jnp.zeros((N, N), F32)
    after, before = both_ways(ca[16:20], cb[16:20], "gx")
    turn[0:4] = after
    turn[N - 4 : N] = before
    turn[...] = turn[...].T
    return mixed


def outer(x, fill=0.0):
    lane = lanes(x.shape[0])
    return jnp.where((lane < 2) | (lane >= N - 2), x, fill)


def side_field(mixed, slot):
    lane = lanes(N)
    moved = mixed if slot == 0 else pltpu.roll(mixed, N - 8 * slot, 1)
    return jnp.where((lane < 4) | (lane >= 124), moved, 0.0)


def root_viscosity(su, sv, st, sh):
    for at in range(TOP - 8, TOP + N + 8, 8):
        here = slice(at, at + 8)
        up, down = slice(at + 1, at + 9), slice(at - 1, at + 7)
        ue, uw = east(su[0, here], su[1, here]), west(su[0, here], su[1, here])
        ve, vw = east(sv[0, here], sv[1, here]), west(sv[0, here], sv[1, here])
        for t in (0, 1):
            strain_xx = 0.5 * (ue[t] - uw[t])
            strain_yy = 0.5 * (sv[t, up] - sv[t, down])
            shear = 0.25 * (su[t, up] - su[t, down] + (ve[t] - vw[t]))
            delta2 = (
                1.25 * (strain_xx * strain_xx + strain_yy * strain_yy)
                + shear * shear
                + 1.5 * strain_xx * strain_yy
            )
            sh[t, here] = jnp.sqrt(st[t, here] / (2.0 * jnp.sqrt(delta2 + DELTA_MIN * DELTA_MIN)))


def systems(su, sv, st, sh, wx, wy, live, tiles, put_u, put_v):
    for at in range(TOP, TOP + N, 8):
        here = slice(at, at + 8)
        up, down = slice(at + 1, at + 9), slice(at - 1, at + 7)
        cell = slice(at - TOP, at - TOP + 8)
        he, hw = east(sh[0, here], sh[1, here]), west(sh[0, here], sh[1, here])
        ve, vw = east(sv[0, here], sv[1, here]), west(sv[0, here], sv[1, here])
        te, tw = east(st[0, here], st[1, here]), west(st[0, here], st[1, here])
        for t in tiles:
            h, thick = sh[t, here], st[t, here]
            e_edge, w_edge = h * he[t], h * hw[t]
            n_edge, s_edge = h * sh[t, up], h * sh[t, down]
            mass = WEAK * thick
            alive = live(t, cell) > 0.5
            if t == 0:
                extra = mass + WEAK * (n_edge + s_edge)
                right = (
                    mass * su[0, here]
                    + DRIVE * wx(cell)
                    + CORIOLIS * mass * sv[0, here]
                    + WEAK * (n_edge * su[0, up] + s_edge * su[0, down])
                    - 0.5 * PRESS * (te[0] - tw[0])
                )
                scale = 1.0 / (extra + e_edge + w_edge)
                put_u(
                    cell,
                    jnp.where(alive, w_edge * scale, 0.0),
                    jnp.where(alive, e_edge * scale, 0.0),
                    jnp.where(alive, extra * scale, 1.0),
                    jnp.where(alive, right * scale, 0.0),
                )
            extra = mass + WEAK * (e_edge + w_edge)
            right = (
                mass * sv[t, here]
                + DRIVE * wy(t, cell)
                + WEAK * (e_edge * ve[t] + w_edge * vw[t])
                - 0.5 * PRESS * (st[t, up] - st[t, down])
            )
            scale = 1.0 / jnp.where(alive, extra + n_edge + s_edge, 1.0)
            put_v(
                t,
                cell,
                jnp.where(alive, s_edge * scale, 0.0),
                jnp.where(alive, n_edge * scale, 0.0),
                jnp.where(alive, extra * scale, 1.0),
                jnp.where(alive, right * scale, 0.0),
                jnp.where(alive, CORIOLIS * mass * scale, 0.0),
            )


def set_rims(bands):
    one, zero = jnp.ones((8, N), F32), jnp.zeros((8, N), F32)
    for half in (0, 1):
        for k in range(4):
            bands[half, k, 0:8] = one if k == 0 else zero
            bands[half, k, 8 + N : 16 + N] = one if k == 1 else zero


def set_band(bands, k, at, value):
    if at + value.shape[0] == N:
        own = sublanes(value.shape[0]) == value.shape[0] - 1
        value = jnp.where(own, 1.0 if k == 1 else 0.0, value)
    bands[0, k, 8 + at : 8 + at + value.shape[0]] = value


def reduce_piece(bands, last, out):
    half, s = 0, 1
    while s < N:
        final = 2 * s >= N
        for at in range(0, N, 8):
            here = slice(8 + at, 16 + at)
            l, u, e, r = (bands[half, k, here] for k in range(4))
            ll, uu, ee, rr = l, u, e, r
            if s < 8 or at >= s:
                low = slice(8 + at - s, 16 + at - s)
                ll = l * bands[half, 0, low]
                ee = ee + l * bands[half, 2, low]
                rr = rr + l * bands[half, 3, low]
            if s < 8 or at + s < N:
                high = slice(8 + at + s, 16 + at + s)
                uu = u * bands[half, 1, high]
                ee = ee + u * bands[half, 2, high]
                rr = rr + u * bands[half, 3, high]
            q = 1.0 / (ll + uu + ee)
            for k, x in enumerate((ll, uu, ee, rr)):
                if final:
                    out(k, at, x * q)
                if not final or at in (0, N - 8):
                    bands[1 - half, k, here] = x * q
        half, s = 1 - half, 2 * s
    row = lambda k, i: bands[half, k, 8 + i : 9 + i]
    lo, uo, eo, ro = last
    lq, uq, eq, rq = (row(k, N - 2) for k in range(4))
    q = 1.0 / (uo + eo + lo * (lq + eq))
    coupling = [row(k, 0) for k in range(4)]
    coupling += [lo * lq * q, uo * q, (eo + lo * eq) * q, (ro + lo * rq) * q]
    second = [row(k, 1) for k in (0, 1, 3)]
    return coupling, second, [lq, uq, rq]


def solve_pieces(take, me, rowed, extra=None):
    fl, fu, fe, fr, zl, zu, ze, zr = (take(k) for k in range(8))
    nxt = lambda a: pltpu.roll(a, K - 1, 0)
    fl, fu, fe, fr = nxt(fl), nxt(fu), nxt(fe), nxt(fr)
    uu, ee, rr = zu * fu, ze + zu * fe, zr + zu * fr
    q = 1.0 / (zl + ee + uu)
    l, u, e, r = zl * q, uu * q, ee * q, rr * q
    s = 1
    while s < K:
        low = lambda a: pltpu.roll(a, s, 0)
        high = lambda a: pltpu.roll(a, K - s, 0)
        ee = e + l * low(e) + u * high(e)
        rr = r + l * low(r) + u * high(r)
        ll, uu = l * low(l), u * high(u)
        q = 1.0 / (ll + uu + ee)
        l, u, e, r = ll * q, uu * q, ee * q, rr * q
        s *= 2
    zero = jnp.zeros((K, N), F32)
    rowed[0:K] = zero
    rowed[K : 2 * K] = r
    rowed[2 * K : 3 * K] = zero
    before, own = rowed[pl.ds(K - 1 + me, 1), :], rowed[pl.ds(K + me, 1), :]
    if extra is None:
        return before, own
    before2, after = rowed[pl.ds(K - 2 + me, 1), :], rowed[pl.ds(K + 1 + me, 1), :]
    rowed[0:K] = jnp.where(sublanes(K) == K - 1, 0.0, fr + fl * r + fu * nxt(r))
    first = rowed[pl.ds(me, 1), :]
    up, down = extra
    second = up(2) + up(0) * own + up(1) * after
    ahead = down(2) + down(0) * before2 + down(1) * before
    return before, own, ahead, first, second


def rows_of(got, width):
    return lambda k: got[pl.ds(k, K, width), :]


def rows_beside(got, width, base, me):
    up = jnp.minimum(me + 1, K - 1) * width + base
    down = jnp.maximum(me - 1, 0) * width + base
    has_up = jnp.broadcast_to(me < K - 1, (1, N))
    has_down = jnp.broadcast_to(me > 0, (1, N))
    return (
        lambda k: jnp.where(has_up, got[pl.ds(up + k, 1), :], 0.0),
        lambda k: jnp.where(has_down, got[pl.ds(down + k, 1), :], 0.0),
    )


def spread(dest, me, common, forward=None, backward=None):
    width = dest.shape[0] // K
    for d in range(K):
        at = d * width
        dest[at : at + 8] = common
        if forward is not None:
            dest[at + 8 : at + width] = pick(me < d, width - 8, forward[: width - 8], backward[: width - 8])


def tile_of(rows, pad):
    for k, row in enumerate(rows):
        pad[k : k + 1] = row
    return pad[...]


def first_u(vel, wind, thick, alive, ra, rb, ca, cb, send, pl_, pu_, pr_, vsys, sth, su, sv, st, sh, turn, tall, bands, pad):
    mixed = side_columns(ca, cb, turn)
    zero = jnp.zeros((TOP, N), F32)
    for k, s in enumerate((su, sv, st)):
        own = vel.at[k] if k < 2 else thick
        for t in (0, 1):
            s[t, 0:TOP] = zero
            s[t, TOP + N :] = zero
            s[t, TOP : TOP + N] = own[...] if t == 0 else side_field(mixed, k)
        above, below = both_ways(ra[k], rb[k], "gy")
        s[0, TOP - 2 : TOP] = below
        s[0, TOP + N : TOP + N + 2] = above
        s[1, TOP - 2 : TOP] = turn[4 * k : 4 * k + 2]
        s[1, TOP + N : TOP + N + 2] = turn[4 * k + 2 : 4 * k + 4]
    tall[0] = side_field(mixed, 3)
    tall[1] = side_field(mixed, 4)
    root_viscosity(su, sv, st, sh)

    def live(t, cell):
        return alive[cell] if t == 0 else tall[1, cell]

    def wy(t, cell):
        return wind[1, cell] if t == 0 else tall[0, cell]

    def put_u(cell, *values):
        for k, x in enumerate(values):
            tall[2 + k, cell] = x

    def put_v(t, cell, *values):
        for k, x in enumerate(values):
            vsys[k, t, cell] = x

    systems(su, sv, st, sh, lambda cell: wind[0, cell], wy, live, (0, 1), put_u, put_v)
    for t in (0, 1):
        sth[t] = st[t]
    last = []
    for k in range(4):
        turned = tall[2 + k].T
        set_band(bands, k, 0, turned)
        last.append(turned[N - 1 :])
    set_rims(bands)
    outs = {0: pl_, 1: pu_, 3: pr_}

    def out(k, at, x):
        if k != 2:
            outs[k][at : at + 8] = x

    main, second, ahead = reduce_piece(bands, last, out)
    me = lax.axis_index("gx")
    common = tile_of(main, pad)
    pad[...] = jnp.zeros((8, N), F32)
    forward = tile_of(ahead, pad)
    backward = tile_of(second, pad)
    spread(send, me, common, forward, backward)


def load_v(bands, vsys, t, speed):
    last = []
    for k in range(4):
        x = vsys[k, t]
        if k == 3:
            x = x - vsys[4, t] * speed
        set_band(bands, k, 0, x)
        last.append(x[N - 1 :])
    set_rims(bands)
    return last


def first_v(got, pl_, pu_, pr_, vsys, send, u_new, vp, turn, bands, pad, rowed):
    me = lax.axis_index("gx")
    before, own, ahead, first, second = solve_pieces(rows_of(got, 11), me, rowed, rows_beside(got, 11, 8, me))
    turn[...] = pr_[...] + pl_[...] * before + pu_[...] * own
    u_new[0] = turn[...].T
    turn[...] = jnp.zeros((N, N), F32)
    turn[0:1] = first
    turn[1:2] = second
    turn[N - 2 : N - 1] = ahead
    turn[N - 1 : N] = before
    u_new[1] = turn[...].T
    for t in (0, 1):
        last = load_v(bands, vsys, t, u_new[t])

        def out(k, at, x):
            if k != 2:
                vp[min(k, 2), t, at : at + 8] = x

        main, second, ahead = reduce_piece(bands, last, out)
        if t == 0:
            common, extras = tile_of(main, pad), (ahead, second)
    packed = jnp.zeros((1, N), F32)
    inward = lambda x, at: pltpu.roll(jnp.where(lanes(1) < 4, pltpu.roll(x, 2, 1), 0.0), at, 1)
    for k, x in enumerate(main):
        packed = packed + (inward(x, 4 * k) if k else jnp.where(lanes(1) < 4, pltpu.roll(x, 2, 1), 0.0))
    pad[...] = jnp.zeros((8, N), F32)
    forward = tile_of(
        [packed + inward(u_new[1, N - 1 : N], 32)] + extras[0] + [u_new[0, N - 2 : N - 1], u_new[0, N - 1 : N]], pad
    )
    backward = tile_of([packed + inward(u_new[1, 0:1], 32)] + extras[1] + [u_new[0, 1:2], u_new[0, 0:1]], pad)
    spread(send, lax.axis_index("gy"), common, forward, backward)


def second_u(got, vp, u_new, sth, wind, alive, send, pl_, pu_, pr_, vsys, su, sv, sh, tall, bands, pad, rowed):
    me = lax.axis_index("gy")
    up, down = rows_beside(got, 16, 8, me)
    coefs = (lambda k: up(1 + k), lambda k: down(1 + k))
    packed = got[pl.ds(8, K, 16), :]
    unpack = lambda k: outer(pltpu.roll(packed, N - 2 - 4 * k, 1), 1.0 if k in (2, 6) else 0.0)
    zero = jnp.zeros((TOP, N), F32)
    for t in (0, 1):
        before, own, ahead, first, second = solve_pieces(rows_of(got, 16) if t == 0 else unpack, me, rowed, coefs)
        for s in (su, sv):
            s[t, 0:TOP] = zero
            s[t, TOP + N :] = zero
        sv[t, TOP : TOP + N] = vp[2, t] + vp[0, t] * before + vp[1, t] * own
        sv[t, TOP - 1 : TOP] = before
        sv[t, TOP + N : TOP + N + 1] = first
        su[t, TOP : TOP + N] = u_new[t]
        if t == 0:
            sv[0, TOP - 2 : TOP - 1] = ahead
            sv[0, TOP + N + 1 : TOP + N + 2] = second
            su[0, TOP - 2 : TOP - 1] = down(4)
            su[0, TOP - 1 : TOP] = down(5)
            su[0, TOP + N : TOP + N + 1] = up(5)
            su[0, TOP + N + 1 : TOP + N + 2] = up(4)
        else:
            su[1, TOP - 1 : TOP] = outer(pltpu.roll(down(0), N - 34, 1))
            su[1, TOP + N : TOP + N + 1] = outer(pltpu.roll(up(0), N - 34, 1))
    root_viscosity(su, sv, sth, sh)

    def live(t, cell):
        return alive[cell]

    def put_u(cell, *values):
        for k, x in enumerate(values):
            tall[k, cell] = x

    def put_v(t, cell, *values):
        for k, x in enumerate(values):
            vsys[k, t, cell] = x

    systems(su, sv, sth, sh, lambda cell: wind[0, cell], lambda t, cell: wind[1, cell], live, (0,), put_u, put_v)
    last = []
    for k in range(4):
        turned = tall[k].T
        set_band(bands, k, 0, turned)
        last.append(turned[N - 1 :])
    set_rims(bands)
    outs = {0: pl_, 1: pu_, 3: pr_}

    def out(k, at, x):
        if k != 2:
            outs[k][at : at + 8] = x

    main, _, _ = reduce_piece(bands, last, out)
    spread(send, lax.axis_index("gx"), tile_of(main, pad))


def second_v(got, pl_, pu_, pr_, vsys, send, u_new, vp, turn, bands, pad, rowed):
    before, own = solve_pieces(rows_of(got, 8), lax.axis_index("gx"), rowed)
    turn[...] = pr_[...] + pl_[...] * before + pu_[...] * own
    u_new[...] = turn[...].T
    last = load_v(bands, vsys, 0, u_new[...])

    def out(k, at, x):
        if k != 2:
            vp[min(k, 2), at : at + 8] = x

    main, _, _ = reduce_piece(bands, last, out)
    spread(send, lax.axis_index("gy"), tile_of(main, pad))


def finish(got, vp, u_new, out, rowed):
    before, own = solve_pieces(rows_of(got, 8), lax.axis_index("gy"), rowed)
    out[0] = u_new[...]
    out[1] = vp[2] + vp[0] * before + vp[1] * own


def call(kernel, outs, scratch, *args, flops=None):
    vmem = pl.BlockSpec(memory_space=pltpu.VMEM)
    shapes = [jax.ShapeDtypeStruct(s, F32) for s in outs]
    cost = None if flops is None else pl.CostEstimate(flops=flops, bytes_accessed=0, transcendentals=0)
    return pl.pallas_call(
        kernel,
        out_shape=shapes,
        in_specs=[vmem] * len(args),
        out_specs=[vmem] * len(outs),
        scratch_shapes=[pltpu.VMEM(s, F32) for s in scratch],
        compiler_params=pltpu.CompilerParams(vmem_limit_bytes=8 * 1024 * 1024),
        cost_estimate=cost,
    )(*args)


def neighbours(a, b, axis):
    inner = [(i, i ^ 1) for i in range(K)]
    outer = [p for i in range(1, K - 1, 2) for p in ((i, i + 1), (i + 1, i))]
    far = lax.ppermute(b, axis, outer)
    near = lax.ppermute(a, axis, inner)
    return near, far


def share(rows, axis):
    width = rows.shape[0] // K
    inside = (width, N) if width % 8 == 0 else (1, width * N)
    moved = lax.all_to_all(rows.reshape(K, *inside), axis, 0, 0, tiled=True)
    return moved.reshape(K * width, N)


def on_device(vel, wind, thick, ice, land):
    square, halves, rim = (N, N), (2, N, N), (2, ROWS, N)
    bands, pad, rowed = (2, 4, N + 16, N), (8, N), (3 * K, N)
    a, b = edge_rows(vel, thick)
    ra, rb = neighbours(a, b, "gy")
    alive = (ice * (1 - land)).astype(F32)
    (edges,) = call(edge_columns, [(32, N)], [square], vel, wind, thick, alive, flops=10**8)
    a, b = call(pack_columns, [(24, N)] * 2, [square], edges, ra, rb)
    ca, cb = neighbours(a, b, "gx")
    send, l, u, r, vsys, sth = call(
        first_u,
        [(K * 11, N), square, square, square, (5,) + halves, rim],
        [rim] * 4 + [square, (6, N, N), bands, pad],
        vel, wind, thick, alive, ra, rb, ca, cb,
    )
    got = share(send, "gx")
    send, u_new, vp = call(
        first_v,
        [(K * 16, N), halves, (3,) + halves],
        [square, bands, pad, rowed],
        got, l, u, r, vsys,
    )
    got = share(send, "gy")
    send, l, u, r, vsys = call(
        second_u,
        [(K * 8, N), square, square, square, (5, 1, N, N)],
        [rim] * 3 + [(4, N, N), bands, pad, rowed],
        got, vp, u_new, sth, wind, alive,
    )
    got = share(send, "gx")
    send, u_new, vp = call(
        second_v,
        [(K * 8, N), square, (3, N, N)],
        [square, bands, pad, rowed],
        got, l, u, r, vsys,
    )
    got = share(send, "gy")
    (out,) = call(finish, [halves], [rowed], got, vp, u_new)
    return out


def solution(mesh):
    field = P(None, "gy", "gx")
    flat = P("gy", "gx")
    return jax.shard_map(
        on_device,
        mesh=mesh,
        in_specs=(field, field, flat, flat, flat),
        out_specs=field,
        check_vma=False,
    )
```

```python
import jax
import jax.numpy as jnp
from jax import lax
from jax.experimental import pallas as pl
from jax.experimental.pallas import tpu as pltpu
from jax.sharding import PartitionSpec as P


CORIOLIS = 1.0
DELTA_MIN = 0.25
WIND_GAIN = 0.2

N = 128
K = 16
TOP = 16
ROWS = N + 2 * TOP
CELLS = float(N * N)
WEAK = 1.0 / (16.0 * CELLS)
PRESS = CELLS ** (-0.25)
DRIVE = WIND_GAIN * CELLS ** (-0.75)
F32 = jnp.float32


def lanes(rows):
    return lax.broadcasted_iota(jnp.int32, (rows, N), 1)


def sublanes(rows):
    return lax.broadcasted_iota(jnp.int32, (rows, N), 0)


def east(own, side):
    a, b = pltpu.roll(own, N - 1, 1), pltpu.roll(side, N - 1, 1)
    last = lanes(own.shape[0]) == N - 1
    return jnp.where(last, b, a), jnp.where(last, a, b)


def west(own, side):
    a, b = pltpu.roll(own, 1, 1), pltpu.roll(side, 1, 1)
    first = lanes(own.shape[0]) == 0
    return jnp.where(first, b, a), jnp.where(first, a, b)


def pick(flag, rows, a, b):
    return jnp.where(jnp.broadcast_to(flag, (rows, N)), a, b)


def edge_rows(vel, thick):
    even = lax.rem(lax.axis_index("gy"), 2) == 0
    fields = jnp.stack([vel[0], vel[1], thick])
    first, final = fields[:, :2], fields[:, N - 2 :]
    return jnp.where(even, final, first), jnp.where(even, first, final)


def edge_columns(vel, wind, thick, alive, edges, turn):
    lane = lanes(N)
    mixed = jnp.where(lane < 36, pltpu.roll(alive[...], 32, 1), vel[0])
    mixed = jnp.where(lane < 28, pltpu.roll(wind[1], 24, 1), mixed)
    mixed = jnp.where(lane < 20, pltpu.roll(thick[...], 16, 1), mixed)
    mixed = jnp.where(lane < 12, pltpu.roll(vel[1], 8, 1), mixed)
    mixed = jnp.where(lane < 4, vel[0], mixed)
    turn[...] = mixed.T
    left = ((0, 4), (8, 4), (16, 4), (24, 2), (32, 2))
    right = ((124, 4), (4, 4), (12, 4), (22, 2), (30, 2))
    for base, places in ((0, left), (16, right)):
        for at, n in places:
            edges[base : base + n] = turn[at : at + n]
            base += n


def both_ways(a, b, axis):
    even = lax.rem(lax.axis_index(axis), 2) == 0
    n = a.shape[0]
    return pick(even, n, a, b), pick(even, n, b, a)


def pack_columns(edges, ra, rb, send_a, send_b, turn):
    turn[...] = jnp.zeros((N, N), F32)
    for k in range(3):
        above, below = both_ways(ra[k], rb[k], "gy")
        turn[4 * k : 4 * k + 2] = below
        turn[4 * k + 2 : 4 * k + 4] = above
    turn[...] = turn[...].T
    even = lax.rem(lax.axis_index("gx"), 2) == 0
    for at, n, left, right in (
        (0, 16, edges[0:16], edges[16:32]),
        (16, 4, turn[0:4], turn[N - 4 : N]),
        (20, 4, jnp.zeros((4, N), F32), jnp.zeros((4, N), F32)),
    ):
        send_a[at : at + n] = pick(even, n, right, left)
        send_b[at : at + n] = pick(even, n, left, right)


def side_columns(ca, cb, turn):
    turn[...] = jnp.zeros((N, N), F32)
    places = ((0, 4, 0, 124), (4, 4, 8, 4), (8, 4, 16, 12), (12, 2, 24, 22), (14, 2, 32, 30))
    for at, n, low, high in places:
        after, before = both_ways(ca[at : at + n], cb[at : at + n], "gx")
        turn[low : low + n] = after
        turn[high : high + n] = before
    mixed = turn[...].T
    turn[...] = jnp.zeros((N, N), F32)
    after, before = both_ways(ca[16:20], cb[16:20], "gx")
    turn[0:4] = after
    turn[N - 4 : N] = before
    turn[...] = turn[...].T
    return mixed


def outer(x, fill=0.0):
    lane = lanes(x.shape[0])
    return jnp.where((lane < 2) | (lane >= N - 2), x, fill)


def side_field(mixed, slot):
    lane = lanes(N)
    moved = mixed if slot == 0 else pltpu.roll(mixed, N - 8 * slot, 1)
    return jnp.where((lane < 4) | (lane >= 124), moved, 0.0)


def root_viscosity(su, sv, st, sh):
    for at in range(TOP - 8, TOP + N + 8, 8):
        here = slice(at, at + 8)
        up, down = slice(at + 1, at + 9), slice(at - 1, at + 7)
        ue, uw = east(su[0, here], su[1, here]), west(su[0, here], su[1, here])
        ve, vw = east(sv[0, here], sv[1, here]), west(sv[0, here], sv[1, here])
        for t in (0, 1):
            strain_xx = 0.5 * (ue[t] - uw[t])
            strain_yy = 0.5 * (sv[t, up] - sv[t, down])
            shear = 0.25 * (su[t, up] - su[t, down] + (ve[t] - vw[t]))
            delta2 = (
                1.25 * (strain_xx * strain_xx + strain_yy * strain_yy)
                + shear * shear
                + 1.5 * strain_xx * strain_yy
            )
            sh[t, here] = jnp.sqrt(0.5 * st[t, here] * lax.rsqrt(delta2 + DELTA_MIN * DELTA_MIN))


def systems(su, sv, st, sh, wx, wy, live, tiles, put_u, put_v):
    for at in range(TOP, TOP + N, 8):
        here = slice(at, at + 8)
        up, down = slice(at + 1, at + 9), slice(at - 1, at + 7)
        cell = slice(at - TOP, at - TOP + 8)
        he, hw = east(sh[0, here], sh[1, here]), west(sh[0, here], sh[1, here])
        ve, vw = east(sv[0, here], sv[1, here]), west(sv[0, here], sv[1, here])
        te, tw = east(st[0, here], st[1, here]), west(st[0, here], st[1, here])
        for t in tiles:
            h, thick = sh[t, here], st[t, here]
            e_edge, w_edge = h * he[t], h * hw[t]
            n_edge, s_edge = h * sh[t, up], h * sh[t, down]
            mass = WEAK * thick
            alive = live(t, cell) > 0.5
            if t == 0:
                extra = mass + WEAK * (n_edge + s_edge)
                right = (
                    mass * su[0, here]
                    + DRIVE * wx(cell)
                    + CORIOLIS * mass * sv[0, here]
                    + WEAK * (n_edge * su[0, up] + s_edge * su[0, down])
                    - 0.5 * PRESS * (te[0] - tw[0])
                )
                scale = 1.0 / (extra + e_edge + w_edge)
                put_u(
                    cell,
                    jnp.where(alive, w_edge * scale, 0.0),
                    jnp.where(alive, e_edge * scale, 0.0),
                    jnp.where(alive, extra * scale, 1.0),
                    jnp.where(alive, right * scale, 0.0),
                )
            extra = mass + WEAK * (e_edge + w_edge)
            right = (
                mass * sv[t, here]
                + DRIVE * wy(t, cell)
                + WEAK * (e_edge * ve[t] + w_edge * vw[t])
                - 0.5 * PRESS * (st[t, up] - st[t, down])
            )
            scale = 1.0 / jnp.where(alive, extra + n_edge + s_edge, 1.0)
            put_v(
                t,
                cell,
                jnp.where(alive, s_edge * scale, 0.0),
                jnp.where(alive, n_edge * scale, 0.0),
                jnp.where(alive, extra * scale, 1.0),
                jnp.where(alive, right * scale, 0.0),
                jnp.where(alive, CORIOLIS * mass * scale, 0.0),
            )


def set_rims(bands):
    one, zero = jnp.ones((8, N), F32), jnp.zeros((8, N), F32)
    for half in (0, 1):
        for k in range(4):
            bands[half, k, 0:8] = one if k == 0 else zero
            bands[half, k, 8 + N : 16 + N] = one if k == 1 else zero


def set_band(bands, k, at, value):
    if at + value.shape[0] == N:
        own = sublanes(value.shape[0]) == value.shape[0] - 1
        value = jnp.where(own, 1.0 if k == 1 else 0.0, value)
    bands[0, k, 8 + at : 8 + at + value.shape[0]] = value


def reduce_level(bands, half, s, at, out):
    here = slice(8 + at, 16 + at)
    l, u, e, r = (bands[half, k, here] for k in range(4))
    ll, uu, ee, rr = l, u, e, r
    if s < 8 or at >= s:
        low = slice(8 + at - s, 16 + at - s)
        ll = l * bands[half, 0, low]
        ee = ee + l * bands[half, 2, low]
        rr = rr + l * bands[half, 3, low]
    if s < 8 or at + s < N:
        high = slice(8 + at + s, 16 + at + s)
        uu = u * bands[half, 1, high]
        ee = ee + u * bands[half, 2, high]
        rr = rr + u * bands[half, 3, high]
    q = 1.0 / (ll + uu + ee)
    final = 2 * s >= N
    for k, x in enumerate((ll, uu, ee, rr)):
        if final and k != 2:
            out(k, at, x * q)
        if not final or at in (0, N - 8):
            bands[1 - half, k, here] = x * q


def reduce_pieces(*pieces):
    half, s = 0, 1
    while s < N:
        for at in range(0, N, 8):
            for bands, _, out in pieces:
                reduce_level(bands, half, s, at, out)
        half, s = 1 - half, 2 * s
    return [coupling_of(bands, half, last) for bands, last, _ in pieces]


def coupling_of(bands, half, last):
    row = lambda k, i: bands[half, k, 8 + i : 9 + i]
    lo, uo, eo, ro = last
    lq, uq, eq, rq = (row(k, N - 2) for k in range(4))
    q = 1.0 / (uo + eo + lo * (lq + eq))
    coupling = [row(k, 0) for k in range(4)]
    coupling += [lo * lq * q, uo * q, (eo + lo * eq) * q, (ro + lo * rq) * q]
    second = [row(k, 1) for k in (0, 1, 3)]
    return coupling, second, [lq, uq, rq]


def solve_pieces(take, me, rowed, extra=None):
    fl, fu, fe, fr, zl, zu, ze, zr = (take(k) for k in range(8))
    nxt = lambda a: pltpu.roll(a, K - 1, 0)
    fl, fu, fe, fr = nxt(fl), nxt(fu), nxt(fe), nxt(fr)
    uu, ee, rr = zu * fu, ze + zu * fe, zr + zu * fr
    q = 1.0 / (zl + ee + uu)
    l, u, e, r = zl * q, uu * q, ee * q, rr * q
    s = 1
    while s < K:
        low = lambda a: pltpu.roll(a, s, 0)
        high = lambda a: pltpu.roll(a, K - s, 0)
        ee = e + l * low(e) + u * high(e)
        rr = r + l * low(r) + u * high(r)
        ll, uu = l * low(l), u * high(u)
        q = 1.0 / (ll + uu + ee)
        l, u, e, r = ll * q, uu * q, ee * q, rr * q
        s *= 2
    zero = jnp.zeros((K, N), F32)
    rowed[0:K] = zero
    rowed[K : 2 * K] = r
    rowed[2 * K : 3 * K] = zero
    before, own = rowed[pl.ds(K - 1 + me, 1), :], rowed[pl.ds(K + me, 1), :]
    if extra is None:
        return before, own
    before2, after = rowed[pl.ds(K - 2 + me, 1), :], rowed[pl.ds(K + 1 + me, 1), :]
    rowed[0:K] = jnp.where(sublanes(K) == K - 1, 0.0, fr + fl * r + fu * nxt(r))
    first = rowed[pl.ds(me, 1), :]
    up, down = extra
    second = up(2) + up(0) * own + up(1) * after
    ahead = down(2) + down(0) * before2 + down(1) * before
    return before, own, ahead, first, second


def rows_of(got, width):
    return lambda k: got[pl.ds(k, K, width), :]


def rows_beside(got, width, base, me):
    up = jnp.minimum(me + 1, K - 1) * width + base
    down = jnp.maximum(me - 1, 0) * width + base
    has_up = jnp.broadcast_to(me < K - 1, (1, N))
    has_down = jnp.broadcast_to(me > 0, (1, N))
    return (
        lambda k: jnp.where(has_up, got[pl.ds(up + k, 1), :], 0.0),
        lambda k: jnp.where(has_down, got[pl.ds(down + k, 1), :], 0.0),
    )


def spread(dest, me, common, forward=None, backward=None):
    width = dest.shape[0] // K
    for d in range(K):
        at = d * width
        dest[at : at + 8] = common
        if forward is not None:
            dest[at + 8 : at + width] = pick(me < d, width - 8, forward[: width - 8], backward[: width - 8])


def tile_of(rows, pad):
    for k, row in enumerate(rows):
        pad[k : k + 1] = row
    return pad[...]


def first_u(vel, wind, thick, alive, ra, rb, ca, cb, send, pl_, pu_, pr_, vsys, sth, su, sv, st, sh, turn, tall, bands, pad):
    mixed = side_columns(ca, cb, turn)
    zero = jnp.zeros((TOP, N), F32)
    for k, s in enumerate((su, sv, st)):
        own = vel.at[k] if k < 2 else thick
        for t in (0, 1):
            s[t, 0:TOP] = zero
            s[t, TOP + N :] = zero
            s[t, TOP : TOP + N] = own[...] if t == 0 else side_field(mixed, k)
        above, below = both_ways(ra[k], rb[k], "gy")
        s[0, TOP - 2 : TOP] = below
        s[0, TOP + N : TOP + N + 2] = above
        s[1, TOP - 2 : TOP] = turn[4 * k : 4 * k + 2]
        s[1, TOP + N : TOP + N + 2] = turn[4 * k + 2 : 4 * k + 4]
    tall[0] = side_field(mixed, 3)
    tall[1] = side_field(mixed, 4)
    root_viscosity(su, sv, st, sh)

    def live(t, cell):
        return alive[cell] if t == 0 else tall[1, cell]

    def wy(t, cell):
        return wind[1, cell] if t == 0 else tall[0, cell]

    def put_u(cell, *values):
        for k, x in enumerate(values):
            tall[2 + k, cell] = x

    def put_v(t, cell, *values):
        for k, x in enumerate(values):
            vsys[k, t, cell] = x

    systems(su, sv, st, sh, lambda cell: wind[0, cell], wy, live, (0, 1), put_u, put_v)
    for t in (0, 1):
        sth[t] = st[t]
    last = []
    for k in range(4):
        turned = tall[2 + k].T
        set_band(bands, k, 0, turned)
        last.append(turned[N - 1 :])
    set_rims(bands)
    outs = {0: pl_, 1: pu_, 3: pr_}

    def out(k, at, x):
        outs[k][at : at + 8] = x

    main, second, ahead = reduce_pieces((bands, last, out))[0]
    me = lax.axis_index("gx")
    common = tile_of(main, pad)
    pad[...] = jnp.zeros((8, N), F32)
    forward = tile_of(ahead, pad)
    backward = tile_of(second, pad)
    spread(send, me, common, forward, backward)


def load_v(bands, vsys, t, speed):
    last = []
    for k in range(4):
        x = vsys[k, t]
        if k == 3:
            x = x - vsys[4, t] * speed
        set_band(bands, k, 0, x)
        last.append(x[N - 1 :])
    set_rims(bands)
    return last


def first_v(got, pl_, pu_, pr_, vsys, send, u_new, vp, turn, bands, bands_outer, pad, rowed):
    me = lax.axis_index("gx")
    before, own, ahead, first, second = solve_pieces(rows_of(got, 11), me, rowed, rows_beside(got, 11, 8, me))
    turn[...] = pr_[...] + pl_[...] * before + pu_[...] * own
    u_new[0] = turn[...].T
    turn[...] = jnp.zeros((N, N), F32)
    turn[0:1] = first
    turn[1:2] = second
    turn[N - 2 : N - 1] = ahead
    turn[N - 1 : N] = before
    u_new[1] = turn[...].T
    pieces = []
    for t, space in enumerate((bands, bands_outer)):

        def out(k, at, x, t=t):
            vp[min(k, 2), t, at : at + 8] = x

        pieces.append((space, load_v(space, vsys, t, u_new[t]), out))
    (main, second, ahead), (outer_main, _, _) = reduce_pieces(*pieces)
    common = tile_of(main, pad)
    packed = jnp.zeros((1, N), F32)
    inward = lambda x, at: pltpu.roll(jnp.where(lanes(1) < 4, pltpu.roll(x, 2, 1), 0.0), at, 1)
    for k, x in enumerate(outer_main):
        packed = packed + (inward(x, 4 * k) if k else jnp.where(lanes(1) < 4, pltpu.roll(x, 2, 1), 0.0))
    pad[...] = jnp.zeros((8, N), F32)
    forward = tile_of(
        [packed + inward(u_new[1, N - 1 : N], 32)] + ahead + [u_new[0, N - 2 : N - 1], u_new[0, N - 1 : N]], pad
    )
    backward = tile_of([packed + inward(u_new[1, 0:1], 32)] + second + [u_new[0, 1:2], u_new[0, 0:1]], pad)
    spread(send, lax.axis_index("gy"), common, forward, backward)


def second_u(got, vp, u_new, sth, wind, alive, send, pl_, pu_, pr_, vsys, su, sv, sh, tall, bands, pad, *rowed):
    me = lax.axis_index("gy")
    up, down = rows_beside(got, 14, 8, me)
    coefs = (lambda k: up(1 + k), lambda k: down(1 + k))
    packed = got[pl.ds(8, K, 14), :]
    unpack = lambda k: outer(pltpu.roll(packed, N - 2 - 4 * k, 1), 1.0 if k in (2, 6) else 0.0)
    zero = jnp.zeros((TOP, N), F32)
    for t in (0, 1):
        before, own, ahead, first, second = solve_pieces(rows_of(got, 14) if t == 0 else unpack, me, rowed[t], coefs)
        for s in (su, sv):
            s[t, 0:TOP] = zero
            s[t, TOP + N :] = zero
        sv[t, TOP : TOP + N] = vp[2, t] + vp[0, t] * before + vp[1, t] * own
        sv[t, TOP - 1 : TOP] = before
        sv[t, TOP + N : TOP + N + 1] = first
        su[t, TOP : TOP + N] = u_new[t]
        if t == 0:
            sv[0, TOP - 2 : TOP - 1] = ahead
            sv[0, TOP + N + 1 : TOP + N + 2] = second
            su[0, TOP - 2 : TOP - 1] = down(4)
            su[0, TOP - 1 : TOP] = down(5)
            su[0, TOP + N : TOP + N + 1] = up(5)
            su[0, TOP + N + 1 : TOP + N + 2] = up(4)
        else:
            su[1, TOP - 1 : TOP] = outer(pltpu.roll(down(0), N - 34, 1))
            su[1, TOP + N : TOP + N + 1] = outer(pltpu.roll(up(0), N - 34, 1))
    root_viscosity(su, sv, sth, sh)

    def live(t, cell):
        return alive[cell]

    def put_u(cell, *values):
        for k, x in enumerate(values):
            tall[k, cell] = x

    def put_v(t, cell, *values):
        for k, x in enumerate(values):
            vsys[k, t, cell] = x

    systems(su, sv, sth, sh, lambda cell: wind[0, cell], lambda t, cell: wind[1, cell], live, (0,), put_u, put_v)
    last = []
    for k in range(4):
        turned = tall[k].T
        set_band(bands, k, 0, turned)
        last.append(turned[N - 1 :])
    set_rims(bands)
    outs = {0: pl_, 1: pu_, 3: pr_}

    def out(k, at, x):
        outs[k][at : at + 8] = x

    main, _, _ = reduce_pieces((bands, last, out))[0]
    spread(send, lax.axis_index("gx"), tile_of(main, pad))


def second_v(got, pl_, pu_, pr_, vsys, send, u_new, vp, turn, bands, pad, rowed):
    before, own = solve_pieces(rows_of(got, 8), lax.axis_index("gx"), rowed)
    turn[...] = pr_[...] + pl_[...] * before + pu_[...] * own
    u_new[...] = turn[...].T
    last = load_v(bands, vsys, 0, u_new[...])

    def out(k, at, x):
        vp[min(k, 2), at : at + 8] = x

    main, _, _ = reduce_pieces((bands, last, out))[0]
    spread(send, lax.axis_index("gy"), tile_of(main, pad))


def finish(got, vp, u_new, out, rowed):
    before, own = solve_pieces(rows_of(got, 8), lax.axis_index("gy"), rowed)
    out[0] = u_new[...]
    out[1] = vp[2] + vp[0] * before + vp[1] * own


def call(kernel, outs, scratch, *args, flops=None):
    vmem = pl.BlockSpec(memory_space=pltpu.VMEM)
    shapes = [jax.ShapeDtypeStruct(s, F32) for s in outs]
    cost = None if flops is None else pl.CostEstimate(flops=flops, bytes_accessed=0, transcendentals=0)
    return pl.pallas_call(
        kernel,
        out_shape=shapes,
        in_specs=[vmem] * len(args),
        out_specs=[vmem] * len(outs),
        scratch_shapes=[pltpu.VMEM(s, F32) for s in scratch],
        compiler_params=pltpu.CompilerParams(vmem_limit_bytes=8 * 1024 * 1024),
        cost_estimate=cost,
    )(*args)


def neighbours(a, b, axis):
    inner = [(i, i ^ 1) for i in range(K)]
    outer = [p for i in range(1, K - 1, 2) for p in ((i, i + 1), (i + 1, i))]
    far = lax.ppermute(b, axis, outer)
    near = lax.ppermute(a, axis, inner)
    return near, far


def share(rows, axis):
    width = rows.shape[0] // K
    inside = (width, N) if width % 8 == 0 else (1, width * N)
    moved = lax.all_to_all(rows.reshape(K, *inside), axis, 0, 0, tiled=True)
    return moved.reshape(K * width, N)


def on_device(vel, wind, thick, ice, land):
    square, halves, rim = (N, N), (2, N, N), (2, ROWS, N)
    bands, pad, rowed = (2, 4, N + 16, N), (8, N), (3 * K, N)
    a, b = edge_rows(vel, thick)
    ra, rb = neighbours(a, b, "gy")
    alive = (ice * (1 - land)).astype(F32)
    (edges,) = call(edge_columns, [(32, N)], [square], vel, wind, thick, alive, flops=10**8)
    a, b = call(pack_columns, [(24, N)] * 2, [square], edges, ra, rb)
    ca, cb = neighbours(a, b, "gx")
    send, l, u, r, vsys, sth = call(
        first_u,
        [(K * 11, N), square, square, square, (5,) + halves, rim],
        [rim] * 4 + [square, (6, N, N), bands, pad],
        vel, wind, thick, alive, ra, rb, ca, cb,
    )
    got = share(send, "gx")
    send, u_new, vp = call(
        first_v,
        [(K * 14, N), halves, (3,) + halves],
        [square, bands, bands, pad, rowed],
        got, l, u, r, vsys,
    )
    got = share(send, "gy")
    send, l, u, r, vsys = call(
        second_u,
        [(K * 8, N), square, square, square, (5, 1, N, N)],
        [rim] * 3 + [(4, N, N), bands, pad, rowed, rowed],
        got, vp, u_new, sth, wind, alive,
    )
    got = share(send, "gx")
    send, u_new, vp = call(
        second_v,
        [(K * 8, N), square, (3, N, N)],
        [square, bands, pad, rowed],
        got, l, u, r, vsys,
    )
    got = share(send, "gy")
    (out,) = call(finish, [halves], [rowed], got, vp, u_new)
    return out


def solution(mesh):
    field = P(None, "gy", "gx")
    flat = P("gy", "gx")
    return jax.shard_map(
        on_device,
        mesh=mesh,
        in_specs=(field, field, flat, flat, flat),
        out_specs=field,
        check_vma=False,
    )
```
